8 devices in a mesh: tp: 2 (over z, y), cp: 4 (over x, core).
Axes of the slice: x: 2, y: 2, z: 1, core: 2. Of those that a mesh axis runs over, the one named last changes fastest.
Arguments:
- x: bfloat16 [8, 2048, 4096], P(None, 'cp')
- grad_out: bfloat16 [8, 2048, 4096], P(None, 'cp')
- norm_gain: bfloat16 [4096], replicated
- w_qkv: bfloat16 [4096, 4608], P(None, 'tp')
- b_qkv: bfloat16 [4608], P('tp')
- w_out: bfloat16 [4096, 4096], P('tp')
- doc_id: int32 [8, 2048], P(None, 'cp')
- pos_in_doc: int32 [8, 2048], P(None, 'cp')
Outputs:
- output 1: bfloat16 [8, 2048, 4096], P(None, 'cp')
- output 2: bfloat16 [8, 2048, 4096], P(None, 'cp')
- output 3: float32 [4096], replicated
- output 4: float32 [4096, 4608], P(None, 'tp')
- output 5: float32 [4608], P('tp')
- output 6: float32 [4096, 4096], P('tp')
All inputs are finite; a program needn't handle non-finite values.
Results may differ from the reference program's by a relative error of at most 0.00824973.
Values are sent between devices in bfloat16 or wider.
A program may use at most 1 GiB of HBM per device.

```python
import jax
import jax.numpy as jnp
from jax import lax

BATCH = 8
SEQ = 2048
D = 4096
HEADS = 32
KV_HEADS = 2
HEAD = 128
QBLK = 64
EPS = 1.5625e-07
ROPE_BASE = 5000000.0


def draw_documents(key):
    cut_points = jax.random.randint(key, (BATCH, 3), 1, SEQ)
    positions = jnp.arange(SEQ, dtype=jnp.int32)
    starts = jnp.any(positions[None, :, None] == cut_points[:, None, :], axis=-1)
    doc_id = jnp.cumsum(starts.astype(jnp.int32), axis=1).astype(jnp.int32)
    first = lax.cummax(jnp.where(starts, positions[None, :], 0), axis=1)
    return doc_id, (positions[None, :] - first).astype(jnp.int32)


def setup_inputs(seed: int = 0) -> dict:
    keys = jax.random.split(jax.random.key(seed), 7)
    width = KV_HEADS * (HEADS // KV_HEADS + 2) * HEAD
    x = jax.random.normal(keys[0], (BATCH, SEQ, D), jnp.float32).astype(jnp.bfloat16)
    grad_out = jax.random.normal(keys[1], (BATCH, SEQ, D), jnp.float32).astype(jnp.bfloat16)
    norm_gain = (1.0 + 0.3 * jax.random.normal(keys[2], (D,), jnp.float32)).astype(jnp.bfloat16)
    w_qkv = (jax.random.normal(keys[3], (D, width), jnp.float32) * D ** -0.5).astype(jnp.bfloat16)
    b_qkv = (0.25 * jax.random.normal(keys[4], (width,), jnp.float32)).astype(jnp.bfloat16)
    w_out = (jax.random.normal(keys[5], (HEADS * HEAD, D), jnp.float32) * (HEADS * HEAD) ** -0.5).astype(jnp.bfloat16)
    doc_id, pos_in_doc = draw_documents(keys[6])
    return {'x': x, 'grad_out': grad_out, 'norm_gain': norm_gain, 'w_qkv': w_qkv, 'b_qkv': b_qkv, 'w_out': w_out, 'doc_id': doc_id, 'pos_in_doc': pos_in_doc}


def rope_tables(pos_in_doc):
    rot_dims = HEAD // 2
    inv_freq = 1.0 / ROPE_BASE ** (jnp.arange(0, rot_dims, 2, dtype=jnp.float32) / rot_dims)
    angles = pos_in_doc.astype(jnp.float32)[..., None] * inv_freq
    return jnp.cos(angles), jnp.sin(angles)


def rotate_pairs(vals, cos_t, sin_t):
    half_rot = cos_t.shape[-1]
    turned_part = vals[..., : 2 * half_rot]
    pairs = turned_part.reshape(turned_part.shape[:-1] + (half_rot, 2))
    even = pairs[..., 0]
    odd = pairs[..., 1]
    turned = jnp.stack([even * cos_t - odd * sin_t, odd * cos_t + even * sin_t], axis=-1)
    return jnp.concatenate([turned.reshape(turned_part.shape), vals[..., 2 * half_rot:]], axis=-1)


def reference(x, grad_out, norm_gain, w_qkv, b_qkv, w_out, doc_id, pos_in_doc):
    per_group = HEADS // KV_HEADS
    scale = HEAD ** -0.5
    tokens = BATCH * SEQ
    n_blocks = SEQ // QBLK
    x_wide = x.astype(jnp.float32)
    inv_rms = lax.rsqrt(jnp.mean(x_wide * x_wide, axis=-1, keepdims=True) + EPS)
    normed = x_wide * inv_rms
    h_in = (normed * norm_gain.astype(jnp.float32)).astype(jnp.bfloat16).reshape(tokens, D)
    qkv_proj = (jnp.dot(h_in, w_qkv, preferred_element_type=jnp.float32) + b_qkv.astype(jnp.float32)).astype(jnp.bfloat16)
    qkv_proj = qkv_proj.reshape(BATCH, SEQ, KV_HEADS, per_group + 2, HEAD)
    cos_t, sin_t = rope_tables(pos_in_doc)
    cos_q = cos_t[:, :, None, None]
    sin_q = sin_t[:, :, None, None]
    cos_k = cos_t[:, :, None]
    sin_k = sin_t[:, :, None]
    q_rot = rotate_pairs(qkv_proj[:, :, :, :per_group].astype(jnp.float32), cos_q, sin_q).astype(jnp.bfloat16).astype(jnp.float32)
    k_rot = rotate_pairs(qkv_proj[:, :, :, per_group].astype(jnp.float32), cos_k, sin_k).astype(jnp.bfloat16).astype(jnp.float32)
    values = qkv_proj[:, :, :, per_group + 1].astype(jnp.float32)
    k_pos = jnp.arange(SEQ)

    def attend_rows(block):
        start = block * QBLK
        q_blk = lax.dynamic_slice_in_dim(q_rot, start, QBLK, axis=1)
        q_doc = lax.dynamic_slice_in_dim(doc_id, start, QBLK, axis=1)
        q_pos = start + jnp.arange(QBLK)
        keep = (q_doc[:, :, None] == doc_id[:, None, :]) & (k_pos[None, None, :] <= q_pos[None, :, None])
        keep = keep[:, :, None, None, :]
        scores = jnp.where(keep, jnp.einsum('bqghe,bsge->bqghs', q_blk, k_rot) * scale, -jnp.inf)
        top = jnp.max(scores, axis=-1, keepdims=True)
        weights = jnp.exp(scores - top)
        probs = weights / jnp.sum(weights, axis=-1, keepdims=True)
        return q_blk, probs

    def fwd_rows(block):
        probs = attend_rows(block)[1]
        return jnp.einsum('bqghs,bsge->bqghe', probs, values)

    context = lax.map(fwd_rows, jnp.arange(n_blocks))
    context = jnp.moveaxis(context, 0, 1).reshape(tokens, HEADS * HEAD).astype(jnp.bfloat16)
    attn = jnp.dot(context, w_out, preferred_element_type=jnp.float32).reshape(BATCH, SEQ, D)
    out = (x_wide + attn).astype(jnp.bfloat16)

    grad_flat = grad_out.reshape(tokens, D)
    grad_w_out = jnp.dot(context.T, grad_flat, preferred_element_type=jnp.float32)
    d_context = jnp.dot(grad_flat, w_out.T, preferred_element_type=jnp.float32).astype(jnp.bfloat16)
    d_heads = d_context.reshape(BATCH, SEQ, KV_HEADS, per_group, HEAD).astype(jnp.float32)
    context_heads = context.reshape(BATCH, SEQ, KV_HEADS, per_group, HEAD).astype(jnp.float32)
    delta = jnp.sum(d_heads * context_heads, axis=-1)

    def bwd_rows(carry, block):
        dk_acc, dv_acc = carry
        q_blk, probs = attend_rows(block)
        start = block * QBLK
        dc_blk = lax.dynamic_slice_in_dim(d_heads, start, QBLK, axis=1)
        delta_blk = lax.dynamic_slice_in_dim(delta, start, QBLK, axis=1)
        d_probs = jnp.einsum('bqghe,bsge->bqghs', dc_blk, values)
        d_scores = probs * (d_probs - delta_blk[..., None])
        dq_blk = scale * jnp.einsum('bqghs,bsge->bqghe', d_scores, k_rot)
        dk_acc = dk_acc + scale * jnp.einsum('bqghs,bqghe->bsge', d_scores, q_blk)
        dv_acc = dv_acc + jnp.einsum('bqghs,bqghe->bsge', probs, dc_blk)
        return (dk_acc, dv_acc), dq_blk

    zero_kv = jnp.zeros((BATCH, SEQ, KV_HEADS, HEAD), jnp.float32)
    (d_keys, d_values), dq_blocks = lax.scan(bwd_rows, (zero_kv, zero_kv), jnp.arange(n_blocks))
    d_queries = jnp.moveaxis(dq_blocks, 0, 1).reshape(BATCH, SEQ, KV_HEADS, per_group, HEAD)
    dq_pre = rotate_pairs(d_queries, cos_q, -sin_q)
    dk_pre = rotate_pairs(d_keys, cos_k, -sin_k)
    d_proj = jnp.concatenate([dq_pre, dk_pre[:, :, :, None], d_values[:, :, :, None]], axis=3).astype(jnp.bfloat16).reshape(tokens, -1)
    grad_b_qkv = jnp.sum(d_proj.astype(jnp.float32), axis=0)
    grad_w_qkv = jnp.dot(h_in.T, d_proj, preferred_element_type=jnp.float32)
    d_hidden = jnp.dot(d_proj, w_qkv.T, preferred_element_type=jnp.float32).reshape(BATCH, SEQ, D)
    grad_gain = jnp.sum(d_hidden * normed, axis=(0, 1))
    d_normed = d_hidden * norm_gain.astype(jnp.float32)
    grad_x = (grad_out.astype(jnp.float32) + inv_rms * (d_normed - normed * jnp.mean(d_normed * normed, axis=-1, keepdims=True))).astype(jnp.bfloat16)
    return out, grad_x, grad_gain, grad_w_qkv, grad_b_qkv, grad_w_out
```

```python
import functools
import math

import jax
import jax.numpy as jnp
from jax import lax
from jax.experimental import pallas as pl
from jax.experimental.pallas import tpu as pltpu
from jax.sharding import PartitionSpec as P


HEAD = 128
ROT = 64
EPS = 1.5625e-07
ROPE_BASE = 5000000.0
TQ = 256
TK = 256
COLS = 512
NEG = -3e38
SCALE = HEAD ** -0.5
SCALE2 = SCALE * math.log2(math.e)
BF = jnp.bfloat16
F32 = jnp.float32
VMEM_ALL = 67043328


def mxu(a, b, contract=((1,), (0,))):
    return lax.dot_general(a, b, (contract, ((), ())), preferred_element_type=F32)


def swap_pairs(v):
    n = v.shape[0]
    even = lax.broadcasted_iota(jnp.int32, v.shape, 0) % 2 == 0
    return jnp.where(even, pltpu.roll(v, n - 1, 0), pltpu.roll(v, 1, 0))


def kernel_call(body, us, grid, in_specs, out_specs, out_shape, args, scratch=(), prefetch=0, alias=None):
    return pl.pallas_call(
        body,
        grid_spec=pltpu.PrefetchScalarGridSpec(
            num_scalar_prefetch=prefetch, grid=grid, in_specs=in_specs, out_specs=out_specs, scratch_shapes=scratch),
        out_shape=out_shape,
        input_output_aliases=alias or {},
        compiler_params=pltpu.CompilerParams(dimension_semantics=("arbitrary",) * len(grid), vmem_limit_bytes=VMEM_ALL),
        cost_estimate=pl.CostEstimate(flops=int(us * 9.96e8), bytes_accessed=int(us * 1e6), transcendentals=0),
    )(*args)


def shape(dims, dtype):
    return jax.ShapeDtypeStruct(dims, dtype)


ANYWHERE = pl.BlockSpec(memory_space=pl.ANY)


def once(dims, column=0):
    return pl.BlockSpec(dims, lambda *_: (0, column), pipeline_mode=pl.Buffered(1))


def rows_of(tm, width, first=0):
    return pl.BlockSpec((tm, width), lambda i, *_: (i + first, 0))


def cols_of(height, tn, first=0):
    return pl.BlockSpec((height, tn), lambda i, *_: (0, i + first))


def tiles_of(dims, nq, b0=0):
    return pl.BlockSpec(dims, lambda b, i, *_: ((b + b0) * nq + i,) + (0,) * (len(dims) - 1))


def tile_cols(height, nq, b0=0):
    return pl.BlockSpec((height, TQ), lambda b, i, *_: (0, (b + b0) * nq + i))


def with_whole(body, n_in, args, in_specs, whole):
    if whole is None:
        return body, {}
    first, extra = len(args), len(whole)
    in_specs += [ANYWHERE] * extra
    args += whole
    return (lambda *refs: body(*refs[:n_in], *refs[n_in + extra:])), {first + u: u for u in range(extra)}


def ride(steps, step_of, quarter, arrays):
    n = steps // 2
    rows, width = arrays[0].shape[0] // n, arrays[0].shape[1]

    def held(slot):
        return pl.BlockSpec((rows, width), lambda *g: (jnp.clip(step_of(*g) - slot * n, 0, n - 1), 0))

    def put(*g):
        return quarter(g[-1][0] % 2 ^ (step_of(*g) // n)) * n + step_of(*g) % n

    return [held(0), held(0), held(1), held(1)], (rows, width), put


def put_sums(step, steps, refs, o_ref):
    for slot in range(2):
        @pl.when(step // (steps // 2) == slot)
        def _():
            o_ref[...] = refs[2 * slot][...] + refs[2 * slot + 1][...]


def head_slice(h):
    return slice(h * HEAD, (h + 1) * HEAD)


def tok_slice(h):
    return slice(h * TQ, (h + 1) * TQ)


def prep_kernel(x_ref, gain_ref, w_ref, b_ref, cos_ref, sin_ref, h_ref, r_ref, kv_ref):
    rows, d = x_ref.shape
    total = jnp.zeros((rows, HEAD), F32)
    for c in range(0, d, HEAD):
        x = x_ref[:, c:c + HEAD].astype(F32)
        total += x * x
    r = lax.rsqrt(jnp.sum(total, axis=1, keepdims=True) * (1.0 / d) + EPS)
    r_ref[...] = r
    for c in range(0, d, HEAD):
        h_ref[:, c:c + HEAD] = (x_ref[:, c:c + HEAD].astype(F32) * r * gain_ref[:, c:c + HEAD]).astype(BF)
    kv = (mxu(h_ref[...], w_ref[...]) + b_ref[...]).astype(BF)
    k = kv[:, :HEAD].T
    top = k[:ROT].astype(F32)
    turned = (top * cos_ref[...] + swap_pairs(top) * sin_ref[...]).astype(BF)
    kv_ref[:, :HEAD] = jnp.concatenate([turned, k[ROT:]], axis=0).T
    kv_ref[:, HEAD:] = kv[:, HEAD:]


def prep(x, gain, w, bias, cos_t, sin_t, qw):
    tokens, d = x.shape
    tm, kv = 256, 2 * HEAD
    row, tab = rows_of(tm, d), cols_of(ROT, tm)
    return kernel_call(
        prep_kernel, 28, (tokens // tm,),
        [row, once((1, d)), once((d, kv), qw // kv), once((1, kv), qw // kv), tab, tab],
        [row, rows_of(tm, 1), rows_of(tm, kv)],
        [shape((tokens, d), BF), shape((tokens, 1), F32), shape((tokens, kv), BF)],
        (x, gain, w, bias, cos_t, sin_t))


def q_kernel(h_ref, w_ref, b_ref, cos_ref, sin_ref, q_ref, qt_ref):
    nq = qt_ref.shape[0]
    for n in range(q_ref.shape[1] // COLS):
        c0 = n * COLS
        p = (mxu(h_ref[...], w_ref[:, c0:c0 + COLS]) + b_ref[:, c0:c0 + COLS]).astype(BF)
        for u in range(4):
            hs = slice(u * HEAD, (u + 1) * HEAD)
            for t in range(nq):
                ts = slice(t * TQ, (t + 1) * TQ)
                tile = p[ts, hs].T
                top = tile[:ROT].astype(F32)
                turned = (top * cos_ref[:, ts] + swap_pairs(top) * sin_ref[:, ts]).astype(BF)
                tile = jnp.concatenate([turned, tile[ROT:]], axis=0)
                qt_ref[t, :, (c0 // HEAD + u) * TQ:(c0 // HEAD + u + 1) * TQ] = tile
                q_ref[ts, c0 + u * HEAD:c0 + (u + 1) * HEAD] = tile.T


def q_turn_kernel(s_ref, h_ref, w_ref, b_ref, cos_ref, sin_ref, rows_ref, q_ref, qt_ref, t_ref, half_ref):
    t = rows_ref[...].T
    t_ref[...] = t

    @pl.when(pl.program_id(0) // (pl.num_programs(0) // 2) == s_ref[0] % 2)
    def _():
        half_ref[...] = t

    q_kernel(h_ref, w_ref, b_ref, cos_ref, sin_ref, q_ref, qt_ref)


def q_project(half, part, parts, whole, h, w, bias, cos_t, sin_t, qw, table=None):
    tokens, d = h.shape
    rows = 512
    nq = rows // TQ
    width = qw // 2
    cols = width // HEAD * TQ
    steps = tokens // rows // parts
    i0 = part * steps
    tab = cols_of(ROT, rows, i0)
    in_specs = [rows_of(rows, d, i0), once((d, width), half), once((1, width), half), tab, tab]
    out_specs = [rows_of(rows, width, i0), pl.BlockSpec((nq, HEAD, cols), lambda i, *_: (i + i0, 0, 0))]
    out_shape = [shape((tokens, width), BF), shape((tokens // TQ, HEAD, cols), BF)]
    args = [h, w, bias, cos_t, sin_t]
    body, alias = with_whole(q_kernel, len(args), args, in_specs, whole)
    if table is not None:
        body, nh, all_w = q_turn_kernel, steps // 2, w.shape[1]
        in_specs.append(rows_of(d // steps, all_w))
        out_specs += [cols_of(all_w, d // steps),
                      pl.BlockSpec((all_w, d // steps), lambda i, s: (0, jnp.clip(i - s[0] % 2 * nh, 0, nh - 1)))]
        out_shape += [shape((all_w, d), BF), shape((all_w, d // 2), BF)]
        args = [table, *args, w]

    return kernel_call(body, 42 // parts, (steps,), in_specs, out_specs, out_shape, args, alias=alias, prefetch=int(table is not None))


def key_bias(start_ref, q0, k0):
    j = k0 + lax.broadcasted_iota(jnp.int32, (TK, TQ), 0)
    i = q0 + lax.broadcasted_iota(jnp.int32, (TK, TQ), 1)
    return jnp.where((j >= start_ref[0]) & (j <= i), 0.0, NEG).astype(F32)


def kv_slots(a_ref, b_ref):
    return ((a_ref, 0, 0), (a_ref, 1, 2), (b_ref, 0, 1), (b_ref, 1, 3))


def kv_spec(chunk, b0=0):
    return pl.BlockSpec((2, 1, chunk, 2 * HEAD), lambda b, *_: (0, b + b0, 0, 0))


def start_spec(b0=0):
    return pl.BlockSpec((1, 1, TQ), lambda b, i, *_: (b + b0, 0, i))


def key_range(s_ref, b, t, nq):
    q0 = s_ref[0] * (nq * TQ) + t * TQ
    return q0, s_ref[1 + b * nq + t] // TK, (q0 + TQ - 1) // TK + 1


def fwd_kernel(s_ref, start_ref, qt_ref, kva_ref, kvb_ref, o_ref, ct_ref, lse_ref, k_s, vt_s, t_s, acc_s, m_s, m8_s, l8_s, e_s):
    b, t, nq = pl.program_id(0), pl.program_id(1), pl.num_programs(1)
    heads = qt_ref.shape[2] // TQ
    chunk = kva_ref.shape[2]

    @pl.when(t == 0)
    def _():
        for ref, i, flip in kv_slots(kva_ref, kvb_ref):
            rows = pl.ds(pl.multiple_of((s_ref[0] ^ flip) * chunk, chunk), chunk)
            k_s[rows, :] = ref[i, 0, :, :HEAD]
            vt_s[:, rows] = ref[i, 0, :, HEAD:].T

    m8_s[...] = jnp.full_like(m8_s, NEG)
    l8_s[...] = jnp.zeros_like(l8_s)
    acc_s[...] = jnp.zeros_like(acc_s)
    q0, lo, hi = key_range(s_ref, b, t, nq)

    def scores(kb, _):
        rows = pl.ds(pl.multiple_of(kb * TK, TK), TK)
        bias = key_bias(start_ref, q0, kb * TK)
        k = k_s[rows, :]
        for h in range(heads):
            sl = tok_slice(h)
            s = mxu(k, qt_ref[0, :, sl]) * SCALE2 + bias
            t_s[rows, sl] = s
            m8_s[:, sl] = jnp.maximum(m8_s[:, sl], jnp.max(s.reshape(TK // 8, 8, TQ), axis=0))
        return 0

    lax.fori_loop(lo, hi, scores, 0)
    m_s[...] = jnp.max(m8_s[...], axis=0, keepdims=True)

    def accumulate(kb, _):
        rows = pl.ds(pl.multiple_of(kb * TK, TK), TK)
        for h in range(heads):
            sl = tok_slice(h)
            e = jnp.exp2(t_s[rows, sl] - m_s[:, sl])
            l8_s[:, sl] += jnp.sum(e.reshape(TK // 8, 8, TQ), axis=0)
            e_s[:, sl] = e.astype(BF)
        acc_s[...] += mxu(vt_s[:, rows], e_s[...])
        return 0

    lax.fori_loop(lo, hi, accumulate, 0)
    l = jnp.sum(l8_s[...], axis=0, keepdims=True)
    lse_ref[0] = m_s[...] + jnp.log2(l)
    l8_s[0:1, :] = 1.0 / l
    for h in range(heads):
        sl = tok_slice(h)
        ct = (acc_s[:, sl] * l8_s[0:1, sl]).astype(BF)
        ct_ref[0, :, sl] = ct
        o_ref[:, head_slice(h)] = ct.T


def attn_fwd(table, start, qt, kva, kvb):
    batch, _, chunk = start.shape
    nq = chunk // TQ
    n, _, cols = qt.shape
    width = cols // TQ * HEAD
    keys = 4 * chunk
    kv, tile = kv_spec(chunk), tiles_of((1, HEAD, cols), nq)
    return kernel_call(
        fwd_kernel, 65, (batch, nq),
        [start_spec(), tile, kv, kv],
        [tiles_of((TQ, width), nq), tile, tiles_of((1, 1, cols), nq)],
        [shape((n * TQ, width), BF), shape((n, HEAD, cols), BF), shape((n, 1, cols), F32)], (table, start, qt, kva, kvb),
        [pltpu.VMEM((keys, HEAD), BF), pltpu.VMEM((HEAD, keys), BF), pltpu.VMEM((keys, cols), F32), pltpu.VMEM((HEAD, cols), F32),
         pltpu.VMEM((1, cols), F32), pltpu.VMEM((8, cols), F32), pltpu.VMEM((8, cols), F32), pltpu.VMEM((TK, cols), BF)],
        prefetch=1)


def bwd_kernel(b0, riding, s_ref, start_ref, qta_ref, qtb_ref, qa_ref, qb_ref, dcta_ref, dctb_ref, cta_ref, ctb_ref, la_ref, lb_ref,
               cos_ref, sin_ref, kva_ref, kvb_ref, *refs):
    nb, nq = pl.num_programs(0), pl.num_programs(1)
    if riding:
        put_sums(pl.program_id(0) * nq + pl.program_id(1), nb * nq, refs[:riding], refs[riding + 5])
    dq_ref, half_ref, dkv0_ref, dkv1_ref, dkvb_ref = refs[riding:riding + 5]
    kv_s, kt_s, dct_s, qd_s, dqt_s, delta_s, pd_s, dkv_s = refs[-8:]
    b, t = pl.program_id(0) + b0, pl.program_id(1)
    heads = dq_ref.shape[1] // HEAD
    chunk = kva_ref.shape[2]

    @pl.when(t == 0)
    def _():
        for ref, i, flip in kv_slots(kva_ref, kvb_ref):
            rows = pl.ds(pl.multiple_of((s_ref[0] ^ flip) * chunk, chunk), chunk)
            kv_s[rows, :] = ref[i, 0]
            kt_s[:, rows] = ref[i, 0, :, :HEAD].T
        dkv_s[...] = jnp.zeros_like(dkv_s)

    def of_head(h, a_ref, b_ref):
        return (a_ref, h) if h < heads // 2 else (b_ref, h - heads // 2)

    for h in range(heads):
        sl = tok_slice(h)
        ref, u = of_head(h, dcta_ref, dctb_ref)
        dct = ref[head_slice(u), :]
        dct_s[:, sl] = dct
        ref, u = of_head(h, qa_ref, qb_ref)
        qd_s[sl, :HEAD] = ref[:, head_slice(u)]
        qd_s[sl, HEAD:] = dct.T
        ref, u = of_head(h, cta_ref, ctb_ref)
        delta_s[:, sl] = jnp.sum(dct.astype(F32) * ref[0, :, tok_slice(u)].astype(F32), axis=0, keepdims=True)
    dqt_s[...] = jnp.zeros_like(dqt_s)
    q0, lo, hi = key_range(s_ref, b, t, nq)

    def step(kb, _):
        rows = pl.ds(pl.multiple_of(kb * TK, TK), TK)
        bias = key_bias(start_ref, q0, kb * TK)
        k = kv_s[rows, :HEAD]
        v = kv_s[rows, HEAD:]
        for h in range(heads):
            sl = tok_slice(h)
            qt, u = of_head(h, qta_ref, qtb_ref)
            lse, _ = of_head(h, la_ref, lb_ref)
            us = tok_slice(u)
            p = jnp.exp2(mxu(k, qt[0, :, us]) * SCALE2 + bias - lse[0, :, us])
            pd_s[TK:, sl] = p.astype(BF)
            pd_s[:TK, sl] = (p * (mxu(v, dct_s[:, sl]) - delta_s[:, sl])).astype(BF)
        dqt_s[...] += mxu(kt_s[:, rows], pd_s[:TK, :])
        both = mxu(pd_s[...], qd_s[...])
        dkv_s[rows, :HEAD] += both[:TK, :HEAD]
        dkv_s[rows, HEAD:] += both[TK:, HEAD:]
        return 0

    lax.fori_loop(lo, hi, step, 0)
    for h in range(heads):
        sl = tok_slice(h)
        top = dqt_s[:ROT, sl] * SCALE
        turned = top * cos_ref[...] - swap_pairs(top) * sin_ref[...]
        dq = jnp.concatenate([turned, dqt_s[ROT:, sl] * SCALE], axis=0).astype(BF).T
        dq_ref[:, head_slice(h)] = dq
        half_ref[:, head_slice(h)] = dq

    @pl.when(t == nq - 1)
    def _():
        for ref, flip in ((dkv0_ref.at[0], 0), (dkv1_ref.at[0], 2), (dkvb_ref.at[0, 0], 1), (dkvb_ref.at[1, 0], 3)):
            rows = pl.ds(pl.multiple_of((s_ref[0] ^ flip) * chunk, chunk), chunk)
            ref[:, :HEAD] = dkv_s[rows, :HEAD] * SCALE
            ref[:, HEAD:] = dkv_s[rows, HEAD:]


def attn_bwd(half, whole, sums, table, start, qts, qs, dcts, cts, lses, cos_t, sin_t, kva, kvb):
    batch, _, chunk = start.shape
    nq = chunk // TQ
    n, _, cols = qts[0].shape
    width = 2 * dcts[0].shape[0]
    keys = 4 * chunk
    nb = batch // 2
    b0 = half * nb
    kv, tile, line = kv_spec(chunk, b0), tiles_of((1, HEAD, cols), nq, b0), tiles_of((1, 1, cols), nq, b0)
    qrow, dct, tab = tiles_of((TQ, width // 2), nq, b0), tile_cols(width // 2, nq, b0), tile_cols(ROT, nq, b0)
    one = shape((nb, chunk, 2 * HEAD), F32)
    one_spec = pl.BlockSpec((1, chunk, 2 * HEAD), lambda b, *_: (b, 0, 0))
    in_specs = [start_spec(b0), tile, tile, qrow, qrow, dct, dct, tile, tile, line, line, tab, tab, kv, kv]
    args = [table, start, *qts, *qs, *dcts, *cts, *lses, cos_t, sin_t, kva, kvb]
    out_specs = [tiles_of((TQ, width), nq, b0), tiles_of((TQ, width), nq), one_spec, one_spec, kv_spec(chunk)]
    out_shape = [shape((n * TQ, width), BF), shape((n * TQ // 2, width), BF), one, one, shape((2, nb, chunk, 2 * HEAD), F32)]
    if sums:
        specs, block, put = ride(nb * nq, lambda b, i, s: b * nq + i, lambda core: core, sums)
        in_specs += specs
        args += sums
        out_specs.append(pl.BlockSpec(block, lambda *g: (put(*g), 0)))
        out_shape.append(shape((4 * sums[0].shape[0], block[1]), F32))
    body, alias = with_whole(functools.partial(bwd_kernel, b0, len(sums)), len(args), args, in_specs, whole)
    return kernel_call(
        body, 80, (nb, nq), in_specs, out_specs, out_shape, args,
        [pltpu.VMEM((keys, 2 * HEAD), BF), pltpu.VMEM((HEAD, keys), BF), pltpu.VMEM((HEAD, 2 * cols), BF), pltpu.VMEM((2 * cols, 2 * HEAD), BF),
         pltpu.VMEM((HEAD, 2 * cols), F32), pltpu.VMEM((1, 2 * cols), F32), pltpu.VMEM((2 * TK, 2 * cols), BF), pltpu.VMEM((keys, 2 * HEAD), F32)],
        prefetch=1, alias=alias)


def first_tile(total, a_s, b_s, w_ref, piece_refs, places, w_s, p_s, sems):
    n = w_s.shape[0] // 256
    part = piece_refs[0].shape[1]

    def copies(k):
        rows = pl.ds(pl.multiple_of(k * 256, 256), 256)
        moves = [(w_ref.at[rows, :], w_s.at[rows, :])]
        moves += [(ref.at[rows, :], p_s.at[rows, pl.ds(pl.multiple_of(c * part, part), part)]) for ref, c in zip(piece_refs, places)]
        return [pltpu.make_async_copy(src, dst, sems.at[u, k]) for u, (src, dst) in enumerate(moves)]

    ahead = 3
    for k in range(ahead):
        for copy in copies(k):
            copy.start()
    total[...] = jnp.zeros_like(total)

    def add(k, _):
        for copy in copies(k):
            copy.wait()

        @pl.when(k + ahead < n)
        def _():
            for copy in copies(k + ahead):
                copy.start()

        rows = pl.ds(pl.multiple_of(k * 256, 256), 256)
        for c in range(0, total.shape[1], COLS):
            cs = slice(c, c + COLS)
            total[:, cs] += mxu(a_s[:, rows], w_s[rows, cs]) + mxu(b_s[:, rows], p_s[rows, cs])
        return 0

    lax.fori_loop(0, n, add, 0)


def out_kernel(s_ref, x_ref, ca_ref, cb_ref, pa_ref, pb_ref, w_ref, p0_ref, p1_ref, p2_ref, p3_ref, *refs):
    put_ref, o_ref, w_s, p_s, c_s, d_s, total_s, sems = refs[-8:]
    put_sums(pl.program_id(0), pl.num_programs(0), refs[:-8], put_ref)
    k = ca_ref.shape[1]
    first = pl.program_id(0) == 0
    c_s[:, :k], c_s[:, k:] = ca_ref[...], cb_ref[...]
    d_s[:, :k], d_s[:, k:] = pa_ref[...], pb_ref[...]

    def finish(cs, acc):
        o_ref[:, cs] = (x_ref[:, cs].astype(F32) + acc).astype(BF)

    tiles = [slice(c, c + COLS) for c in range(0, o_ref.shape[1], COLS)]

    @pl.when(first)
    def _():
        first_tile(total_s, c_s, d_s, w_ref, (p0_ref, p1_ref, p2_ref, p3_ref), [s_ref[0] ^ flip for flip in (0, 2, 1, 3)], w_s, p_s, sems)
        for cs in tiles:
            finish(cs, total_s[:, cs])

    @pl.when(jnp.logical_not(first))
    def _():
        for cs in tiles:
            finish(cs, mxu(c_s[...], w_s[:, cs]) + mxu(d_s[...], p_s[:, cs]))


def out_project(table, x, ctx, peer, w, pieces, sums, whole):
    tokens, d = x.shape
    k = w.shape[0]
    tm = 256
    n = tokens // tm
    row, crow = rows_of(tm, d), rows_of(tm, k // 2)
    specs, block, put = ride(n, lambda i, s: i, lambda core: 2 + core, sums)
    in_specs = [row, crow, crow, crow, crow] + [ANYWHERE] * 5 + specs
    args = [table, x, *ctx, *peer, w, *pieces, *sums]
    body, alias = with_whole(out_kernel, len(args), args, in_specs, [whole])
    return kernel_call(
        body, 150, (n,), in_specs, [pl.BlockSpec(block, lambda *g: (put(*g), 0)), row],
        [shape(whole.shape, F32), shape((tokens, d), BF)], args,
        [pltpu.VMEM((k, d), BF), pltpu.VMEM((k, d), BF), pltpu.VMEM((tm, k), BF), pltpu.VMEM((tm, k), BF), pltpu.VMEM((tm, d), F32),
         pltpu.SemaphoreType.DMA((5, k // 256))], prefetch=1, alias=alias)


def finish_kernel(a_ref, b_ref, c_ref, cos_ref, sin_ref, o_ref):
    dkv = a_ref[0] + b_ref[0, 0] + c_ref[0]
    k = dkv[:, :HEAD].T
    top = k[:ROT]
    turned = top * cos_ref[...] - swap_pairs(top) * sin_ref[...]
    o_ref[:, :HEAD] = jnp.concatenate([turned, k[ROT:]], axis=0).T.astype(BF)
    o_ref[:, HEAD:] = dkv[:, HEAD:].astype(BF)


def finish_dkv(half, own, core, away, cos_t, sin_t):
    nb, chunk, width = own.shape
    one = pl.BlockSpec((1, chunk, width), lambda b: (b, 0, 0))
    tab = cols_of(ROT, chunk, half * nb)
    return kernel_call(
        finish_kernel, 4, (nb,), [one, kv_spec(chunk), one, tab, tab], rows_of(chunk, width),
        shape((nb * chunk, width), BF), (own, core, away, cos_t, sin_t))


def dh_kernel(s_ref, x_ref, g_ref, r_ref, gain_ref, qa_ref, ka_ref, qb_ref, kb_ref, w_ref, p0_ref, p1_ref,
              gx_ref, gg_ref, gb_ref, dh_s, gg8_s, gb8_s, w_s, p_s, a_s, b_s, sems):
    i = pl.program_id(0)
    qw = qa_ref.shape[1]
    tm, d = x_ref.shape
    a_s[:, :qw], a_s[:, qw:] = qa_ref[...], ka_ref[...]
    b_s[:, :qw], b_s[:, qw:] = qb_ref[...], kb_ref[...]

    @pl.when(i == 0)
    def _():
        gg8_s[...] = jnp.zeros_like(gg8_s)
        gb8_s[...] = jnp.zeros_like(gb8_s)
        core = s_ref[0] % 2
        first_tile(dh_s, a_s, b_s, w_ref, (p0_ref, p1_ref), (core, 1 - core), w_s, p_s, sems)

    @pl.when(i > 0)
    def _():
        for c in range(0, d, COLS):
            cs = slice(c, c + COLS)
            dh_s[:, cs] = mxu(a_s[...], w_s[:, cs]) + mxu(b_s[...], p_s[:, cs])

    def norm(k, _):
        n = 128
        rs = pl.ds(pl.multiple_of(k * n, n), n)
        r = jnp.broadcast_to(r_ref[rs, :], (n, HEAD))
        total = jnp.zeros((n, HEAD), F32)
        for c in range(0, d, HEAD):
            cs = slice(c, c + HEAD)
            prod = dh_s[rs, cs] * (x_ref[rs, cs].astype(F32) * r)
            gg8_s[:, cs] += jnp.sum(prod.reshape(n // 8, 8, HEAD), axis=0)
            total += prod * gain_ref[:, cs]
        mean = jnp.sum(total, axis=1, keepdims=True) * (1.0 / d)
        r_mean = jnp.broadcast_to(r_ref[rs, :] * mean, (n, HEAD))
        for c in range(0, d, HEAD):
            cs = slice(c, c + HEAD)
            part_x = dh_s[rs, cs] * gain_ref[:, cs] - x_ref[rs, cs].astype(F32) * r_mean
            gx_ref[rs, cs] = (g_ref[rs, cs].astype(F32) + r * part_x).astype(BF)
        for c in range(0, a_s.shape[1], HEAD):
            cs = slice(c, c + HEAD)
            gb8_s[:, cs] += jnp.sum(a_s[rs, cs].astype(F32).reshape(n // 8, 8, HEAD), axis=0)
        return 0

    lax.fori_loop(0, tm // 128, norm, 0)

    @pl.when(i == pl.num_programs(0) - 1)
    def _():
        gg_ref[...] = jnp.sum(gg8_s[...], axis=0, keepdims=True)
        gb_ref[...] = jnp.sum(gb8_s[...], axis=0, keepdims=True)


def dh_norm(half, whole, table, x, g, r, gain, qa, ka, qb, kb, wt, pieces):
    tokens, d = x.shape
    tm = 256
    nt = tokens // tm // 2
    i0 = half * nt
    qw, kw = qa.shape[1], ka.shape[1]
    row = rows_of(tm, d, i0)
    in_specs = [row, row, rows_of(tm, 1, i0), once((1, d)), rows_of(tm, qw, i0), rows_of(tm, kw), rows_of(tm, qw), rows_of(tm, kw)] + [ANYWHERE] * 3
    args = [table, x, g, r, gain, qa, ka, qb, kb, wt, *pieces]
    body, alias = with_whole(dh_kernel, len(args), args, in_specs, whole)
    all_w = qw + kw
    return kernel_call(
        body, 100, (nt,), in_specs, [row, once((1, d)), once((1, all_w))],
        [shape((tokens, d), BF), shape((1, d), F32), shape((1, all_w), F32)], args,
        [pltpu.VMEM((tm, d), F32), pltpu.VMEM((8, d), F32), pltpu.VMEM((8, all_w), F32), pltpu.VMEM((all_w, d), BF), pltpu.VMEM((all_w, d), BF),
         pltpu.VMEM((tm, all_w), BF), pltpu.VMEM((tm, all_w), BF), pltpu.SemaphoreType.DMA((3, all_w // 256))],
        prefetch=1, alias=alias)


def place_kernel(s_ref, a_ref, b_ref, c_ref, d_ref, o_ref):
    put_sums(pl.program_id(0), pl.num_programs(0), (a_ref, b_ref, c_ref, d_ref), o_ref)


def place(table, sums, quarter, column, whole, dims):
    steps = 8
    in_specs, block, put = ride(steps, lambda i, s: i, quarter, sums)
    args = [table, *sums]
    body, alias = with_whole(place_kernel, len(args), args, in_specs, whole)
    return kernel_call(
        body, 20, (steps,), in_specs, pl.BlockSpec(block, lambda *g: (put(*g), column)), shape(dims, F32), args, prefetch=1, alias=alias)


def solution(mesh):
    over_tp = [(i, 1 - i) for i in range(2)]
    over_x = [(i, i ^ 2) for i in range(4)]
    over_core = [(i, i ^ 1) for i in range(4)]

    def send_tp(v):
        return lax.ppermute(v, 'tp', over_tp)

    def send_x(v, pairs=over_x):
        return lax.ppermute(v, 'cp', pairs)

    def send_core(v):
        return lax.ppermute(v, 'cp', over_core)

    def body(x_blk, grad_blk, norm_gain, w_qkv, b_qkv, w_out, doc_blk, pos_blk):
        batch, chunk, d = x_blk.shape
        tokens = batch * chunk
        qw = w_out.shape[0]
        cp = lax.axis_index('cp')
        core = cp % 2
        x = x_blk.reshape(tokens, d)
        g = grad_blk.reshape(tokens, d)
        gain = norm_gain[None].astype(F32)
        bias = b_qkv[None].astype(F32)

        start = cp * chunk + jnp.arange(chunk, dtype=jnp.int32)[None] - pos_blk
        table = jnp.concatenate([cp[None].astype(jnp.int32), start[:, ::TQ].reshape(-1)])
        start = start[:, None, :]
        me = table[:1]

        inv_freq = 1.0 / ROPE_BASE ** (jnp.arange(0, ROT, 2, dtype=F32) / ROT)
        angles = pos_blk.reshape(1, tokens).astype(F32) * jnp.repeat(inv_freq, 2)[:, None]
        sign = jnp.where(jnp.arange(ROT) % 2 == 0, -1.0, 1.0)[:, None]
        cos_t = jnp.cos(angles)
        sin_t = jnp.sin(angles) * sign

        wo0 = send_tp(lax.dynamic_slice_in_dim(w_out, cp * (d // 4), d // 4, 1))
        h, inv_rms, kv = prep(x, gain, w_qkv, bias, cos_t, sin_t, qw)
        kv_own = kv.reshape(batch, chunk, 2 * HEAD)
        kva = jnp.stack([kv_own, send_x(kv_own, over_x[:2])])
        kvb = send_core(kva)
        q_args = (h, w_qkv, bias, cos_t, sin_t, qw)
        qa, qta, wq_t, wq_half = q_project(0, 0, 1, None, *q_args, table=me)
        wq0 = send_tp(wq_half)
        wo1 = send_x(wo0)
        wo_pieces = (wo0, wo1, send_core(wo0), send_core(wo1))
        wq_pieces = (wq0, send_core(wq0))

        ctx_a, ct_a, lse_a = attn_fwd(table, start, qta, kva, kvb)
        qb, qtb = q_project(1, 1, 2, q_project(1, 0, 2, None, *q_args), *q_args)
        ctx_b, ct_b, lse_b = attn_fwd(table, start, qtb, kva, kvb)
        peer_ctx = (send_tp(ctx_a), send_tp(ctx_b))

        def part(lhs, rhs, first, k):
            cols = lax.dynamic_slice_in_dim(lhs, first * k, k, 1)
            return lax.dot_general(cols, rhs, (((0,), (0,)), ((), ())), preferred_element_type=F32)

        def across(v):
            other = send_x(v)
            return [v, other, send_core(v), send_core(other)]

        go = []
        for ctx in (ctx_a, ctx_b):
            k = ctx.shape[1] // 2
            got = send_core(part(ctx, g, 1 - core, k))
            mine = part(ctx, g, core, k) + got
            go.append(across(mine))

        def grad_ctx(w):
            return lax.dot_general(w, g, (((1,), (1,)), ((), ())), preferred_element_type=F32).astype(BF)

        dctx_t = (grad_ctx(w_out[:qw // 2]), grad_ctx(w_out[qw // 2:]))

        attn_args = (table, start, (qta, qtb), (qa, qb), dctx_t, (ct_a, ct_b), (lse_a, lse_b), cos_t, sin_t, kva, kvb)

        def own_dkv(half, own, away, others):
            got = send_core(others)
            return finish_dkv(half, own, got, send_x(away + got[1], over_x[2:]), cos_t, sin_t)

        dq, dq_a, *dkv_parts, gw_out = attn_bwd(0, None, go[0], *attn_args)
        dqp_a = send_tp(dq_a)
        dkv_a = own_dkv(0, *dkv_parts)
        dq, dq_b, *dkv_parts = attn_bwd(1, [dq], [], *attn_args)
        dqp_b = send_tp(dq_b)
        dkv_b = own_dkv(1, *dkv_parts)
        dkvp_a = send_tp(dkv_a)
        dkvp_b = send_tp(dkv_b)
        dkv = jnp.concatenate([dkv_a, dkv_b], axis=0)

        k = d // 4
        got = [send_core(part(h, dq, 2 * (1 - core) + i, k)) for i in range(2)]
        mine = [part(h, dq, 2 * core + i, k) + got[i] for i in range(2)]
        gq = [across(mine[i]) for i in range(2)]
        got = send_core(part(h, dkv, 1 - core, 2 * k))
        gkv = across(part(h, dkv, core, 2 * k) + got)
        dims = (d, w_qkv.shape[1])
        gw_qkv = place(me, gq[0], lambda core: 2 * core, 0, None, dims)
        gw_qkv = place(me, gq[1], lambda core: 2 * core + 1, 0, [gw_qkv], dims)
        gw_qkv = place(me, gkv, lambda core: core, qw // gkv[0].shape[1], [gw_qkv], dims)

        gw_out, out = out_project(me, x, (ctx_a, ctx_b), peer_ctx, w_out, wo_pieces, go[1], gw_out)

        dh_args = (me, x, g, inv_rms, gain, dq)
        grad_x, gain_a, bias_a = dh_norm(0, None, *dh_args, dkv_a, dqp_a, dkvp_a, wq_t, wq_pieces)
        grad_x, gain_b, bias_b = dh_norm(1, [grad_x], *dh_args, dkv_b, dqp_b, dkvp_b, wq_t, wq_pieces)
        nb = bias_a.shape[1]
        small = jnp.concatenate([bias_a + bias_b, gain_a + gain_b], axis=1).reshape(-1, HEAD)
        small = small + send_core(small)
        small = (small + send_x(small)).reshape(-1)
        return out.reshape(x_blk.shape), grad_x.reshape(x_blk.shape), small[nb:], gw_qkv, small[:nb], gw_out

    seq, rep, cols = P(None, 'cp', None), P(), P(None, 'tp')
    specs_in = (seq, seq, rep, cols, P('tp'), P('tp', None), P(None, 'cp'), P(None, 'cp'))
    specs_out = (seq, seq, rep, cols, P('tp'), P('tp', None))
    return jax.shard_map(body, mesh=mesh, in_specs=specs_in, out_specs=specs_out, check_vma=False)
```

```python
import functools
import math

import jax
import jax.numpy as jnp
from jax import lax
from jax.experimental import pallas as pl
from jax.experimental.pallas import tpu as pltpu
from jax.sharding import PartitionSpec as P


HEAD = 128
ROT = 64
EPS = 1.5625e-07
ROPE_BASE = 5000000.0
TQ = 256
TK = 256
COLS = 512
NEG = -3e38
SCALE = HEAD ** -0.5
SCALE2 = SCALE * math.log2(math.e)
BF = jnp.bfloat16
F32 = jnp.float32
VMEM_ALL = 67043328


def mxu(a, b, contract=((1,), (0,))):
    return lax.dot_general(a, b, (contract, ((), ())), preferred_element_type=F32)


def swap_pairs(v):
    n = v.shape[0]
    even = lax.broadcasted_iota(jnp.int32, v.shape, 0) % 2 == 0
    return jnp.where(even, pltpu.roll(v, n - 1, 0), pltpu.roll(v, 1, 0))


def kernel_call(body, us, grid, in_specs, out_specs, out_shape, args, scratch=(), prefetch=0, alias=None):
    return pl.pallas_call(
        body,
        grid_spec=pltpu.PrefetchScalarGridSpec(
            num_scalar_prefetch=prefetch, grid=grid, in_specs=in_specs, out_specs=out_specs, scratch_shapes=scratch),
        out_shape=out_shape,
        input_output_aliases=alias or {},
        compiler_params=pltpu.CompilerParams(dimension_semantics=("arbitrary",) * len(grid), vmem_limit_bytes=VMEM_ALL),
        cost_estimate=pl.CostEstimate(flops=int(us * 9.96e8), bytes_accessed=int(us * 1e6), transcendentals=0),
    )(*args)


def shape(dims, dtype):
    return jax.ShapeDtypeStruct(dims, dtype)


ANYWHERE = pl.BlockSpec(memory_space=pl.ANY)


def once(dims, column=0):
    return pl.BlockSpec(dims, lambda *_: (0, column), pipeline_mode=pl.Buffered(1))


def rows_of(tm, width, first=0):
    return pl.BlockSpec((tm, width), lambda i, *_: (i + first, 0))


def cols_of(height, tn, first=0):
    return pl.BlockSpec((height, tn), lambda i, *_: (0, i + first))


def tiles_of(dims, nq, b0=0):
    return pl.BlockSpec(dims, lambda b, i, *_: ((b + b0) * nq + i,) + (0,) * (len(dims) - 1))


def tile_cols(height, nq, b0=0):
    return pl.BlockSpec((height, TQ), lambda b, i, *_: (0, (b + b0) * nq + i))


def with_whole(body, n_in, args, in_specs, whole):
    if whole is None:
        return body, {}
    first, extra = len(args), len(whole)
    in_specs += [ANYWHERE] * extra
    args += whole
    return (lambda *refs: body(*refs[:n_in], *refs[n_in + extra:])), {first + u: u for u in range(extra)}


def ride(steps, step_of, quarter, arrays):
    n = steps // 2
    rows, width = arrays[0].shape[0] // n, arrays[0].shape[1]

    def held(slot):
        return pl.BlockSpec((rows, width), lambda *g: (jnp.clip(step_of(*g) - slot * n, 0, n - 1), 0))

    def put(*g):
        return quarter(g[-1][0] % 2 ^ (step_of(*g) // n)) * n + step_of(*g) % n

    return [held(0), held(0), held(1), held(1)], (rows, width), put


def put_sums(step, steps, refs, o_ref):
    for slot in range(2):
        @pl.when(step // (steps // 2) == slot)
        def _():
            o_ref[...] = refs[2 * slot][...] + refs[2 * slot + 1][...]


def head_slice(h):
    return slice(h * HEAD, (h + 1) * HEAD)


def tok_slice(h):
    return slice(h * TQ, (h + 1) * TQ)


def prep_kernel(x_ref, gain_ref, w_ref, b_ref, cos_ref, sin_ref, h_ref, r_ref, kv_ref):
    rows, d = x_ref.shape
    total = jnp.zeros((rows, HEAD), F32)
    for c in range(0, d, HEAD):
        x = x_ref[:, c:c + HEAD].astype(F32)
        total += x * x
    r = lax.rsqrt(jnp.sum(total, axis=1, keepdims=True) * (1.0 / d) + EPS)
    r_ref[...] = r
    for c in range(0, d, HEAD):
        h_ref[:, c:c + HEAD] = (x_ref[:, c:c + HEAD].astype(F32) * r * gain_ref[:, c:c + HEAD]).astype(BF)
    kv = (mxu(h_ref[...], w_ref[...]) + b_ref[...]).astype(BF)
    k = kv[:, :HEAD].T
    top = k[:ROT].astype(F32)
    turned = (top * cos_ref[...] + swap_pairs(top) * sin_ref[...]).astype(BF)
    kv_ref[:, :HEAD] = jnp.concatenate([turned, k[ROT:]], axis=0).T
    kv_ref[:, HEAD:] = kv[:, HEAD:]


def prep(x, gain, w, bias, cos_t, sin_t, qw):
    tokens, d = x.shape
    tm, kv = 256, 2 * HEAD
    row, tab = rows_of(tm, d), cols_of(ROT, tm)
    return kernel_call(
        prep_kernel, 28, (tokens // tm,),
        [row, once((1, d)), once((d, kv), qw // kv), once((1, kv), qw // kv), tab, tab],
        [row, rows_of(tm, 1), rows_of(tm, kv)],
        [shape((tokens, d), BF), shape((tokens, 1), F32), shape((tokens, kv), BF)],
        (x, gain, w, bias, cos_t, sin_t))


def q_kernel(h_ref, w_ref, b_ref, cos_ref, sin_ref, qt_ref):
    nq = qt_ref.shape[0]
    for n in range(w_ref.shape[1] // COLS):
        c0 = n * COLS
        p = (mxu(h_ref[...], w_ref[:, c0:c0 + COLS]) + b_ref[:, c0:c0 + COLS]).astype(BF)
        for u in range(4):
            hs = slice(u * HEAD, (u + 1) * HEAD)
            for t in range(nq):
                ts = slice(t * TQ, (t + 1) * TQ)
                tile = p[ts, hs].T
                top = tile[:ROT].astype(F32)
                turned = (top * cos_ref[:, ts] + swap_pairs(top) * sin_ref[:, ts]).astype(BF)
                sl = tok_slice(c0 // HEAD + u)
                qt_ref[t, :ROT, sl] = turned
                qt_ref[t, ROT:, sl] = tile[ROT:]


def q_turn_kernel(s_ref, h_ref, w_ref, b_ref, cos_ref, sin_ref, rows_ref, qt_ref, t_ref, half_ref):
    t = rows_ref[...].T
    t_ref[...] = t

    @pl.when(pl.program_id(0) // (pl.num_programs(0) // 2) == s_ref[0] % 2)
    def _():
        half_ref[...] = t

    q_kernel(h_ref, w_ref, b_ref, cos_ref, sin_ref, qt_ref)


def q_project(half, part, parts, whole, h, w, bias, cos_t, sin_t, qw, table=None):
    tokens, d = h.shape
    rows = 512
    nq = rows // TQ
    width = qw // 2
    cols = width // HEAD * TQ
    steps = tokens // rows // parts
    i0 = part * steps
    tab = cols_of(ROT, rows, i0)
    in_specs = [rows_of(rows, d, i0), once((d, width), half), once((1, width), half), tab, tab]
    out_specs = [pl.BlockSpec((nq, HEAD, cols), lambda i, *_: (i + i0, 0, 0))]
    out_shape = [shape((tokens // TQ, HEAD, cols), BF)]
    args = [h, w, bias, cos_t, sin_t]
    body, alias = with_whole(q_kernel, len(args), args, in_specs, whole)
    if table is not None:
        body, nh, all_w = q_turn_kernel, steps // 2, w.shape[1]
        in_specs.append(rows_of(d // steps, all_w))
        out_specs += [cols_of(all_w, d // steps),
                      pl.BlockSpec((all_w, d // steps), lambda i, s: (0, jnp.clip(i - s[0] % 2 * nh, 0, nh - 1)))]
        out_shape += [shape((all_w, d), BF), shape((all_w, d // 2), BF)]
        args = [table, *args, w]

    return kernel_call(body, 42 // parts, (steps,), in_specs, out_specs, out_shape, args, alias=alias, prefetch=int(table is not None))


def for_keys(lo, hi, step):
    def pair(i, _):
        step(pl.multiple_of((lo + 2 * i) * TK, TK), 2 * TK)
        return 0

    lax.fori_loop(0, (hi - lo) // 2, pair, 0)

    @pl.when((hi - lo) % 2 == 1)
    def _():
        step(pl.multiple_of((hi - 1) * TK, TK), TK)


def key_bias(start_ref, q0, k0, n):
    j = k0 + lax.broadcasted_iota(jnp.int32, (n, TQ), 0)
    i = q0 + lax.broadcasted_iota(jnp.int32, (n, TQ), 1)
    return jnp.where((j >= start_ref[0]) & (j <= i), 0.0, NEG).astype(F32)


def kv_slots(a_ref, b_ref):
    return ((a_ref, 0, 0), (a_ref, 1, 2), (b_ref, 0, 1), (b_ref, 1, 3))


def kv_spec(chunk, b0=0):
    return pl.BlockSpec((2, 1, chunk, 2 * HEAD), lambda b, *_: (0, b + b0, 0, 0))


def start_spec(b0=0):
    return pl.BlockSpec((1, 1, TQ), lambda b, i, *_: (b + b0, 0, i))


def key_range(s_ref, b, t, nq):
    q0 = s_ref[0] * (nq * TQ) + t * TQ
    return q0, s_ref[1 + b * nq + t] // TK, (q0 + TQ - 1) // TK + 1


def fwd_kernel(s_ref, start_ref, qt_ref, kva_ref, kvb_ref, o_ref, ct_ref, lse_ref, k_s, vt_s, t_s, acc_s, m_s, m8_s, l8_s, e_s):
    b, t, nq = pl.program_id(0), pl.program_id(1), pl.num_programs(1)
    heads = qt_ref.shape[2] // TQ
    chunk = kva_ref.shape[2]

    @pl.when(t == 0)
    def _():
        for ref, i, flip in kv_slots(kva_ref, kvb_ref):
            rows = pl.ds(pl.multiple_of((s_ref[0] ^ flip) * chunk, chunk), chunk)
            k_s[rows, :] = ref[i, 0, :, :HEAD]
            vt_s[:, rows] = ref[i, 0, :, HEAD:].T

    m8_s[...] = jnp.full_like(m8_s, NEG)
    l8_s[...] = jnp.zeros_like(l8_s)
    acc_s[...] = jnp.zeros_like(acc_s)
    q0, lo, hi = key_range(s_ref, b, t, nq)

    def scores(k0, n):
        rows = pl.ds(k0, n)
        bias = key_bias(start_ref, q0, k0, n)
        k = k_s[rows, :]
        for h in range(heads):
            sl = tok_slice(h)
            s = mxu(k, qt_ref[0, :, sl]) * SCALE2 + bias
            t_s[rows, sl] = s
            m8_s[:, sl] = jnp.maximum(m8_s[:, sl], jnp.max(s.reshape(n // 8, 8, TQ), axis=0))

    for_keys(lo, hi, scores)
    m_s[...] = jnp.max(m8_s[...], axis=0, keepdims=True)

    def accumulate(k0, n):
        rows = pl.ds(k0, n)
        for h in range(heads):
            sl = tok_slice(h)
            e = jnp.exp2(t_s[rows, sl] - m_s[:, sl])
            l8_s[:, sl] += jnp.sum(e.reshape(n // 8, 8, TQ), axis=0)
            e_s[:n, sl] = e.astype(BF)
        acc_s[...] += mxu(vt_s[:, rows], e_s[:n, :])

    for_keys(lo, hi, accumulate)
    l = jnp.sum(l8_s[...], axis=0, keepdims=True)
    lse_ref[0] = m_s[...] + jnp.log2(l)
    l8_s[0:1, :] = 1.0 / l
    for h in range(heads):
        sl = tok_slice(h)
        ct = (acc_s[:, sl] * l8_s[0:1, sl]).astype(BF)
        ct_ref[0, :, sl] = ct
        o_ref[:, head_slice(h)] = ct.T


def attn_fwd(table, start, qt, kva, kvb):
    batch, _, chunk = start.shape
    nq = chunk // TQ
    n, _, cols = qt.shape
    width = cols // TQ * HEAD
    keys = 4 * chunk
    kv, tile = kv_spec(chunk), tiles_of((1, HEAD, cols), nq)
    return kernel_call(
        fwd_kernel, 65, (batch, nq),
        [start_spec(), tile, kv, kv],
        [tiles_of((TQ, width), nq), tile, tiles_of((1, 1, cols), nq)],
        [shape((n * TQ, width), BF), shape((n, HEAD, cols), BF), shape((n, 1, cols), F32)], (table, start, qt, kva, kvb),
        [pltpu.VMEM((keys, HEAD), BF), pltpu.VMEM((HEAD, keys), BF), pltpu.VMEM((keys, cols), F32), pltpu.VMEM((HEAD, cols), F32),
         pltpu.VMEM((1, cols), F32), pltpu.VMEM((8, cols), F32), pltpu.VMEM((8, cols), F32), pltpu.VMEM((2 * TK, cols), BF)],
        prefetch=1)


def bwd_kernel(b0, riding, s_ref, start_ref, qta_ref, qtb_ref, dcta_ref, dctb_ref, cta_ref, ctb_ref, la_ref, lb_ref,
               cos_ref, sin_ref, kva_ref, kvb_ref, *refs):
    nb, nq = pl.num_programs(0), pl.num_programs(1)
    if riding:
        put_sums(pl.program_id(0) * nq + pl.program_id(1), nb * nq, refs[:riding], refs[riding + 5])
    dq_ref, half_ref, dkv0_ref, dkv1_ref, dkvb_ref = refs[riding:riding + 5]
    kv_s, kt_s, dct_s, dqt_s, delta_s, ds_s, dsn_s, pn_s, dkvt_s = refs[-9:]
    b, t = pl.program_id(0) + b0, pl.program_id(1)
    heads = dq_ref.shape[1] // HEAD
    chunk = kva_ref.shape[2]

    @pl.when(t == 0)
    def _():
        for ref, i, flip in kv_slots(kva_ref, kvb_ref):
            rows = pl.ds(pl.multiple_of((s_ref[0] ^ flip) * chunk, chunk), chunk)
            kv_s[rows, :] = ref[i, 0]
            kt_s[:, rows] = ref[i, 0, :, :HEAD].T
        dkvt_s[...] = jnp.zeros_like(dkvt_s)

    def of_head(h, a_ref, b_ref):
        return (a_ref, h) if h < heads // 2 else (b_ref, h - heads // 2)

    for h in range(heads):
        sl = tok_slice(h)
        ref, u = of_head(h, dcta_ref, dctb_ref)
        dct = ref[head_slice(u), :]
        dct_s[:, sl] = dct
        ref, u = of_head(h, cta_ref, ctb_ref)
        delta_s[:, sl] = jnp.sum(dct.astype(F32) * ref[0, :, tok_slice(u)].astype(F32), axis=0, keepdims=True)
    dqt_s[...] = jnp.zeros_like(dqt_s)
    q0, lo, hi = key_range(s_ref, b, t, nq)

    def step(kb, _):
        k0 = pl.multiple_of(kb * TK, TK)
        rows = pl.ds(k0, TK)
        bias = key_bias(start_ref, q0, k0, TK)
        k = kv_s[rows, :HEAD]
        v = kv_s[rows, HEAD:]
        for h in range(heads):
            sl = tok_slice(h)
            qt, u = of_head(h, qta_ref, qtb_ref)
            lse, _ = of_head(h, la_ref, lb_ref)
            us = tok_slice(u)
            p = jnp.exp2(mxu(k, qt[0, :, us]) * SCALE2 + bias - lse[0, :, us])
            ds = (p * (mxu(v, dct_s[:, sl]) - delta_s[:, sl])).astype(BF)
            pn_s[sl, :] = p.astype(BF).T
            dsn_s[sl, :] = ds.T
            ds_s[:, sl] = ds
        dqt_s[...] += mxu(kt_s[:, rows], ds_s[...])
        half = dsn_s.shape[0] // 2
        dkvt_s[:HEAD, rows] += mxu(qta_ref[0], dsn_s[:half, :]) + mxu(qtb_ref[0], dsn_s[half:, :])
        dkvt_s[HEAD:, rows] += mxu(dct_s[...], pn_s[...])
        return 0

    lax.fori_loop(lo, hi, step, 0)
    for h in range(heads):
        sl = tok_slice(h)
        top = dqt_s[:ROT, sl] * SCALE
        turned = top * cos_ref[...] - swap_pairs(top) * sin_ref[...]
        dq = jnp.concatenate([turned, dqt_s[ROT:, sl] * SCALE], axis=0).astype(BF).T
        dq_ref[:, head_slice(h)] = dq
        half_ref[:, head_slice(h)] = dq

    @pl.when(t == nq - 1)
    def _():
        for ref, flip in ((dkv0_ref.at[0], 0), (dkv1_ref.at[0], 2), (dkvb_ref.at[0, 0], 1), (dkvb_ref.at[1, 0], 3)):
            rows = pl.ds(pl.multiple_of((s_ref[0] ^ flip) * chunk, chunk), chunk)
            ref[:, :HEAD] = (dkvt_s[:HEAD, rows] * SCALE).T
            ref[:, HEAD:] = dkvt_s[HEAD:, rows].T


def attn_bwd(half, whole, sums, table, start, qts, dcts, cts, lses, cos_t, sin_t, kva, kvb):
    batch, _, chunk = start.shape
    nq = chunk // TQ
    n, _, cols = qts[0].shape
    width = 2 * dcts[0].shape[0]
    keys = 4 * chunk
    nb = batch // 2
    b0 = half * nb
    kv, tile, line = kv_spec(chunk, b0), tiles_of((1, HEAD, cols), nq, b0), tiles_of((1, 1, cols), nq, b0)
    dct, tab = tile_cols(width // 2, nq, b0), tile_cols(ROT, nq, b0)
    one = shape((nb, chunk, 2 * HEAD), F32)
    one_spec = pl.BlockSpec((1, chunk, 2 * HEAD), lambda b, *_: (b, 0, 0))
    in_specs = [start_spec(b0), tile, tile, dct, dct, tile, tile, line, line, tab, tab, kv, kv]
    args = [table, start, *qts, *dcts, *cts, *lses, cos_t, sin_t, kva, kvb]
    out_specs = [tiles_of((TQ, width), nq, b0), tiles_of((TQ, width), nq), one_spec, one_spec, kv_spec(chunk)]
    out_shape = [shape((n * TQ, width), BF), shape((n * TQ // 2, width), BF), one, one, shape((2, nb, chunk, 2 * HEAD), F32)]
    if sums:
        specs, block, put = ride(nb * nq, lambda b, i, s: b * nq + i, lambda core: core, sums)
        in_specs += specs
        args += sums
        out_specs.append(pl.BlockSpec(block, lambda *g: (put(*g), 0)))
        out_shape.append(shape((4 * sums[0].shape[0], block[1]), F32))
    body, alias = with_whole(functools.partial(bwd_kernel, b0, len(sums)), len(args), args, in_specs, whole)
    return kernel_call(
        body, 80, (nb, nq), in_specs, out_specs, out_shape, args,
        [pltpu.VMEM((keys, 2 * HEAD), BF), pltpu.VMEM((HEAD, keys), BF), pltpu.VMEM((HEAD, 2 * cols), BF),
         pltpu.VMEM((HEAD, 2 * cols), F32), pltpu.VMEM((1, 2 * cols), F32), pltpu.VMEM((TK, 2 * cols), BF),
         pltpu.VMEM((2 * cols, TK), BF), pltpu.VMEM((2 * cols, TK), BF), pltpu.VMEM((2 * HEAD, keys), F32)],
        prefetch=1, alias=alias)


def first_tile(total, a_s, b_s, w_ref, piece_refs, places, w_s, p_s, sems):
    n = w_s.shape[0] // 256
    part = piece_refs[0].shape[1]

    def copies(k):
        rows = pl.ds(pl.multiple_of(k * 256, 256), 256)
        moves = [(w_ref.at[rows, :], w_s.at[rows, :])]
        moves += [(ref.at[rows, :], p_s.at[rows, pl.ds(pl.multiple_of(c * part, part), part)]) for ref, c in zip(piece_refs, places)]
        return [pltpu.make_async_copy(src, dst, sems.at[u, k]) for u, (src, dst) in enumerate(moves)]

    ahead = 3
    for k in range(ahead):
        for copy in copies(k):
            copy.start()
    total[...] = jnp.zeros_like(total)

    def add(k, _):
        for copy in copies(k):
            copy.wait()

        @pl.when(k + ahead < n)
        def _():
            for copy in copies(k + ahead):
                copy.start()

        rows = pl.ds(pl.multiple_of(k * 256, 256), 256)
        for c in range(0, total.shape[1], COLS):
            cs = slice(c, c + COLS)
            total[:, cs] += mxu(a_s[:, rows], w_s[rows, cs]) + mxu(b_s[:, rows], p_s[rows, cs])
        return 0

    lax.fori_loop(0, n, add, 0)


def out_kernel(s_ref, x_ref, ca_ref, cb_ref, pa_ref, pb_ref, w_ref, p0_ref, p1_ref, p2_ref, p3_ref, *refs):
    put_ref, o_ref, w_s, p_s, c_s, d_s, total_s, sems = refs[-8:]
    put_sums(pl.program_id(0), pl.num_programs(0), refs[:-8], put_ref)
    k = ca_ref.shape[1]
    first = pl.program_id(0) == 0
    c_s[:, :k], c_s[:, k:] = ca_ref[...], cb_ref[...]
    d_s[:, :k], d_s[:, k:] = pa_ref[...], pb_ref[...]

    def finish(cs, acc):
        o_ref[:, cs] = (x_ref[:, cs].astype(F32) + acc).astype(BF)

    tiles = [slice(c, c + COLS) for c in range(0, o_ref.shape[1], COLS)]

    @pl.when(first)
    def _():
        first_tile(total_s, c_s, d_s, w_ref, (p0_ref, p1_ref, p2_ref, p3_ref), [s_ref[0] ^ flip for flip in (0, 2, 1, 3)], w_s, p_s, sems)
        for cs in tiles:
            finish(cs, total_s[:, cs])

    @pl.when(jnp.logical_not(first))
    def _():
        for cs in tiles:
            finish(cs, mxu(c_s[...], w_s[:, cs]) + mxu(d_s[...], p_s[:, cs]))


def out_project(table, x, ctx, peer, w, pieces, sums, whole):
    tokens, d = x.shape
    k = w.shape[0]
    tm = 256
    n = tokens // tm
    row, crow = rows_of(tm, d), rows_of(tm, k // 2)
    specs, block, put = ride(n, lambda i, s: i, lambda core: 2 + core, sums)
    in_specs = [row, crow, crow, crow, crow] + [ANYWHERE] * 5 + specs
    args = [table, x, *ctx, *peer, w, *pieces, *sums]
    body, alias = with_whole(out_kernel, len(args), args, in_specs, [whole])
    return kernel_call(
        body, 150, (n,), in_specs, [pl.BlockSpec(block, lambda *g: (put(*g), 0)), row],
        [shape(whole.shape, F32), shape((tokens, d), BF)], args,
        [pltpu.VMEM((k, d), BF), pltpu.VMEM((k, d), BF), pltpu.VMEM((tm, k), BF), pltpu.VMEM((tm, k), BF), pltpu.VMEM((tm, d), F32),
         pltpu.SemaphoreType.DMA((5, k // 256))], prefetch=1, alias=alias)


def finish_kernel(a_ref, b_ref, c_ref, cos_ref, sin_ref, o_ref):
    dkv = a_ref[0] + b_ref[0, 0] + c_ref[0]
    k = dkv[:, :HEAD].T
    top = k[:ROT]
    turned = top * cos_ref[...] - swap_pairs(top) * sin_ref[...]
    o_ref[:, :HEAD] = jnp.concatenate([turned, k[ROT:]], axis=0).T.astype(BF)
    o_ref[:, HEAD:] = dkv[:, HEAD:].astype(BF)


def finish_dkv(half, own, core, away, cos_t, sin_t):
    nb, chunk, width = own.shape
    one = pl.BlockSpec((1, chunk, width), lambda b: (b, 0, 0))
    tab = cols_of(ROT, chunk, half * nb)
    return kernel_call(
        finish_kernel, 4, (nb,), [one, kv_spec(chunk), one, tab, tab], rows_of(chunk, width),
        shape((nb * chunk, width), BF), (own, core, away, cos_t, sin_t))


def dh_kernel(s_ref, x_ref, g_ref, r_ref, gain_ref, qa_ref, ka_ref, qb_ref, kb_ref, w_ref, p0_ref, p1_ref,
              gx_ref, gg_ref, gb_ref, dh_s, gg8_s, gb8_s, w_s, p_s, a_s, b_s, sems):
    i = pl.program_id(0)
    qw = qa_ref.shape[1]
    tm, d = x_ref.shape
    a_s[:, :qw], a_s[:, qw:] = qa_ref[...], ka_ref[...]
    b_s[:, :qw], b_s[:, qw:] = qb_ref[...], kb_ref[...]

    @pl.when(i == 0)
    def _():
        gg8_s[...] = jnp.zeros_like(gg8_s)
        gb8_s[...] = jnp.zeros_like(gb8_s)
        core = s_ref[0] % 2
        first_tile(dh_s, a_s, b_s, w_ref, (p0_ref, p1_ref), (core, 1 - core), w_s, p_s, sems)

    @pl.when(i > 0)
    def _():
        for c in range(0, d, COLS):
            cs = slice(c, c + COLS)
            dh_s[:, cs] = mxu(a_s[...], w_s[:, cs]) + mxu(b_s[...], p_s[:, cs])

    def norm(k, _):
        n = 128
        rs = pl.ds(pl.multiple_of(k * n, n), n)
        r = jnp.broadcast_to(r_ref[rs, :], (n, HEAD))
        total = jnp.zeros((n, HEAD), F32)
        for c in range(0, d, HEAD):
            cs = slice(c, c + HEAD)
            prod = dh_s[rs, cs] * (x_ref[rs, cs].astype(F32) * r)
            gg8_s[:, cs] += jnp.sum(prod.reshape(n // 8, 8, HEAD), axis=0)
            total += prod * gain_ref[:, cs]
        mean = jnp.sum(total, axis=1, keepdims=True) * (1.0 / d)
        r_mean = jnp.broadcast_to(r_ref[rs, :] * mean, (n, HEAD))
        for c in range(0, d, HEAD):
            cs = slice(c, c + HEAD)
            part_x = dh_s[rs, cs] * gain_ref[:, cs] - x_ref[rs, cs].astype(F32) * r_mean
            gx_ref[rs, cs] = (g_ref[rs, cs].astype(F32) + r * part_x).astype(BF)
        for c in range(0, a_s.shape[1], HEAD):
            cs = slice(c, c + HEAD)
            gb8_s[:, cs] += jnp.sum(a_s[rs, cs].astype(F32).reshape(n // 8, 8, HEAD), axis=0)
        return 0

    lax.fori_loop(0, tm // 128, norm, 0)

    @pl.when(i == pl.num_programs(0) - 1)
    def _():
        gg_ref[...] = jnp.sum(gg8_s[...], axis=0, keepdims=True)
        gb_ref[...] = jnp.sum(gb8_s[...], axis=0, keepdims=True)


def dh_norm(half, whole, table, x, g, r, gain, qa, ka, qb, kb, wt, pieces):
    tokens, d = x.shape
    tm = 256
    nt = tokens // tm // 2
    i0 = half * nt
    qw, kw = qa.shape[1], ka.shape[1]
    row = rows_of(tm, d, i0)
    in_specs = [row, row, rows_of(tm, 1, i0), once((1, d)), rows_of(tm, qw, i0), rows_of(tm, kw), rows_of(tm, qw), rows_of(tm, kw)] + [ANYWHERE] * 3
    args = [table, x, g, r, gain, qa, ka, qb, kb, wt, *pieces]
    body, alias = with_whole(dh_kernel, len(args), args, in_specs, whole)
    all_w = qw + kw
    return kernel_call(
        body, 100, (nt,), in_specs, [row, once((1, d)), once((1, all_w))],
        [shape((tokens, d), BF), shape((1, d), F32), shape((1, all_w), F32)], args,
        [pltpu.VMEM((tm, d), F32), pltpu.VMEM((8, d), F32), pltpu.VMEM((8, all_w), F32), pltpu.VMEM((all_w, d), BF), pltpu.VMEM((all_w, d), BF),
         pltpu.VMEM((tm, all_w), BF), pltpu.VMEM((tm, all_w), BF), pltpu.SemaphoreType.DMA((3, all_w // 256))],
        prefetch=1, alias=alias)


def place_kernel(s_ref, a_ref, b_ref, c_ref, d_ref, o_ref):
    put_sums(pl.program_id(0), pl.num_programs(0), (a_ref, b_ref, c_ref, d_ref), o_ref)


def place(table, sums, quarter, column, whole, dims):
    steps = 8
    in_specs, block, put = ride(steps, lambda i, s: i, quarter, sums)
    args = [table, *sums]
    body, alias = with_whole(place_kernel, len(args), args, in_specs, whole)
    return kernel_call(
        body, 20, (steps,), in_specs, pl.BlockSpec(block, lambda *g: (put(*g), column)), shape(dims, F32), args, prefetch=1, alias=alias)


def solution(mesh):
    over_tp = [(i, 1 - i) for i in range(2)]
    over_x = [(i, i ^ 2) for i in range(4)]
    over_core = [(i, i ^ 1) for i in range(4)]

    def send_tp(v):
        return lax.ppermute(v, 'tp', over_tp)

    def send_x(v, pairs=over_x):
        return lax.ppermute(v, 'cp', pairs)

    def send_core(v):
        return lax.ppermute(v, 'cp', over_core)

    def body(x_blk, grad_blk, norm_gain, w_qkv, b_qkv, w_out, doc_blk, pos_blk):
        batch, chunk, d = x_blk.shape
        tokens = batch * chunk
        qw = w_out.shape[0]
        cp = lax.axis_index('cp')
        core = cp % 2
        x = x_blk.reshape(tokens, d)
        g = grad_blk.reshape(tokens, d)
        gain = norm_gain[None].astype(F32)
        bias = b_qkv[None].astype(F32)

        start = cp * chunk + jnp.arange(chunk, dtype=jnp.int32)[None] - pos_blk
        table = jnp.concatenate([cp[None].astype(jnp.int32), start[:, ::TQ].reshape(-1)])
        start = start[:, None, :]
        me = table[:1]

        inv_freq = 1.0 / ROPE_BASE ** (jnp.arange(0, ROT, 2, dtype=F32) / ROT)
        angles = pos_blk.reshape(1, tokens).astype(F32) * jnp.repeat(inv_freq, 2)[:, None]
        sign = jnp.where(jnp.arange(ROT) % 2 == 0, -1.0, 1.0)[:, None]
        cos_t = jnp.cos(angles)
        sin_t = jnp.sin(angles) * sign

        wo0 = send_tp(lax.dynamic_slice_in_dim(w_out, cp * (d // 4), d // 4, 1))
        h, inv_rms, kv = prep(x, gain, w_qkv, bias, cos_t, sin_t, qw)
        kv_own = kv.reshape(batch, chunk, 2 * HEAD)
        kva = jnp.stack([kv_own, send_x(kv_own, over_x[:2])])
        kvb = send_core(kva)
        q_args = (h, w_qkv, bias, cos_t, sin_t, qw)
        qta, wq_t, wq_half = q_project(0, 0, 1, None, *q_args, table=me)
        wq0 = send_tp(wq_half)
        wo1 = send_x(wo0)
        wo_pieces = (wo0, wo1, send_core(wo0), send_core(wo1))
        wq_pieces = (wq0, send_core(wq0))

        ctx_a, ct_a, lse_a = attn_fwd(table, start, qta, kva, kvb)
        qtb, = q_project(1, 1, 2, q_project(1, 0, 2, None, *q_args), *q_args)
        ctx_b, ct_b, lse_b = attn_fwd(table, start, qtb, kva, kvb)
        peer_ctx = (send_tp(ctx_a), send_tp(ctx_b))

        def part(lhs, rhs, first, k):
            cols = lax.dynamic_slice_in_dim(lhs, first * k, k, 1)
            return lax.dot_general(cols, rhs, (((0,), (0,)), ((), ())), preferred_element_type=F32)

        def across(v):
            other = send_x(v)
            return [v, other, send_core(v), send_core(other)]

        go = []
        for ctx in (ctx_a, ctx_b):
            k = ctx.shape[1] // 2
            got = send_core(part(ctx, g, 1 - core, k))
            mine = part(ctx, g, core, k) + got
            go.append(across(mine))

        def grad_ctx(w):
            return lax.dot_general(w, g, (((1,), (1,)), ((), ())), preferred_element_type=F32).astype(BF)

        dctx_t = (grad_ctx(w_out[:qw // 2]), grad_ctx(w_out[qw // 2:]))

        attn_args = (table, start, (qta, qtb), dctx_t, (ct_a, ct_b), (lse_a, lse_b), cos_t, sin_t, kva, kvb)

        def own_dkv(half, own, away, others):
            got = send_core(others)
            return finish_dkv(half, own, got, send_x(away + got[1], over_x[2:]), cos_t, sin_t)

        dq, dq_a, *dkv_parts, gw_out = attn_bwd(0, None, go[0], *attn_args)
        dqp_a = send_tp(dq_a)
        dkv_a = own_dkv(0, *dkv_parts)
        dq, dq_b, *dkv_parts = attn_bwd(1, [dq], [], *attn_args)
        dqp_b = send_tp(dq_b)
        dkv_b = own_dkv(1, *dkv_parts)
        dkvp_a = send_tp(dkv_a)
        dkvp_b = send_tp(dkv_b)
        dkv = jnp.concatenate([dkv_a, dkv_b], axis=0)

        k = d // 4
        got = [send_core(part(h, dq, 2 * (1 - core) + i, k)) for i in range(2)]
        mine = [part(h, dq, 2 * core + i, k) + got[i] for i in range(2)]
        gq = [across(mine[i]) for i in range(2)]
        got = send_core(part(h, dkv, 1 - core, 2 * k))
        gkv = across(part(h, dkv, core, 2 * k) + got)
        dims = (d, w_qkv.shape[1])
        gw_qkv = place(me, gq[0], lambda core: 2 * core, 0, None, dims)
        gw_qkv = place(me, gq[1], lambda core: 2 * core + 1, 0, [gw_qkv], dims)
        gw_qkv = place(me, gkv, lambda core: core, qw // gkv[0].shape[1], [gw_qkv], dims)

        gw_out, out = out_project(me, x, (ctx_a, ctx_b), peer_ctx, w_out, wo_pieces, go[1], gw_out)

        dh_args = (me, x, g, inv_rms, gain, dq)
        grad_x, gain_a, bias_a = dh_norm(0, None, *dh_args, dkv_a, dqp_a, dkvp_a, wq_t, wq_pieces)
        grad_x, gain_b, bias_b = dh_norm(1, [grad_x], *dh_args, dkv_b, dqp_b, dkvp_b, wq_t, wq_pieces)
        nb = bias_a.shape[1]
        small = jnp.concatenate([bias_a + bias_b, gain_a + gain_b], axis=1).reshape(-1, HEAD)
        small = small + send_core(small)
        small = (small + send_x(small)).reshape(-1)
        return out.reshape(x_blk.shape), grad_x.reshape(x_blk.shape), small[nb:], gw_qkv, small[:nb], gw_out

    seq, rep, cols = P(None, 'cp', None), P(), P(None, 'tp')
    specs_in = (seq, seq, rep, cols, P('tp'), P('tp', None), P(None, 'cp'), P(None, 'cp'))
    specs_out = (seq, seq, rep, cols, P('tp'), P('tp', None))
    return jax.shard_map(body, mesh=mesh, in_specs=specs_in, out_specs=specs_out, check_vma=False)
```

```python
import functools
import math

import jax
import jax.numpy as jnp
from jax import lax
from jax.experimental import pallas as pl
from jax.experimental.pallas import tpu as pltpu
from jax.sharding import PartitionSpec as P


HEAD = 128
ROT = 64
EPS = 1.5625e-07
ROPE_BASE = 5000000.0
TQ = 256
TK = 256
COLS = 512
NEG = -3e38
SCALE = HEAD ** -0.5
SCALE2 = SCALE * math.log2(math.e)
BF = jnp.bfloat16
F32 = jnp.float32
VMEM_ALL = 67043328


def mxu(a, b, contract=((1,), (0,))):
    return lax.dot_general(a, b, (contract, ((), ())), preferred_element_type=F32)


def swap_pairs(v):
    n = v.shape[0]
    even = lax.broadcasted_iota(jnp.int32, v.shape, 0) % 2 == 0
    return jnp.where(even, pltpu.roll(v, n - 1, 0), pltpu.roll(v, 1, 0))


def kernel_call(body, us, grid, in_specs, out_specs, out_shape, args, scratch=(), prefetch=0, alias=None):
    return pl.pallas_call(
        body,
        grid_spec=pltpu.PrefetchScalarGridSpec(
            num_scalar_prefetch=prefetch, grid=grid, in_specs=in_specs, out_specs=out_specs, scratch_shapes=scratch),
        out_shape=out_shape,
        input_output_aliases=alias or {},
        compiler_params=pltpu.CompilerParams(dimension_semantics=("arbitrary",) * len(grid), vmem_limit_bytes=VMEM_ALL),
        cost_estimate=pl.CostEstimate(flops=int(us * 9.96e8), bytes_accessed=int(us * 1e6), transcendentals=0),
    )(*args)


def shape(dims, dtype):
    return jax.ShapeDtypeStruct(dims, dtype)


ANYWHERE = pl.BlockSpec(memory_space=pl.ANY)


def once(dims, column=0):
    return pl.BlockSpec(dims, lambda *_: (0, column), pipeline_mode=pl.Buffered(1))


def rows_of(tm, width, first=0):
    return pl.BlockSpec((tm, width), lambda i, *_: (i + first, 0))


def cols_of(height, tn, first=0):
    return pl.BlockSpec((height, tn), lambda i, *_: (0, i + first))


def tiles_of(dims, nq, b0=0):
    return pl.BlockSpec(dims, lambda b, i, *_: ((b + b0) * nq + i,) + (0,) * (len(dims) - 1))


def tile_cols(height, nq, b0=0):
    return pl.BlockSpec((height, TQ), lambda b, i, *_: (0, (b + b0) * nq + i))


def with_whole(body, n_in, args, in_specs, whole):
    if whole is None:
        return body, {}
    first, extra = len(args), len(whole)
    in_specs += [ANYWHERE] * extra
    args += whole
    return (lambda *refs: body(*refs[:n_in], *refs[n_in + extra:])), {first + u: u for u in range(extra)}


def ride(steps, step_of, quarter, arrays):
    n = steps // 2
    rows, width = arrays[0].shape[0] // n, arrays[0].shape[1]

    def held(slot):
        return pl.BlockSpec((rows, width), lambda *g: (jnp.clip(step_of(*g) - slot * n, 0, n - 1), 0))

    def put(*g):
        return quarter(g[-1][0] % 2 ^ (step_of(*g) // n)) * n + step_of(*g) % n

    return [held(0), held(0), held(1), held(1)], (rows, width), put


def put_sums(step, steps, refs, o_ref):
    for slot in range(2):
        @pl.when(step // (steps // 2) == slot)
        def _():
            o_ref[...] = refs[2 * slot][...] + refs[2 * slot + 1][...]


def head_slice(h):
    return slice(h * HEAD, (h + 1) * HEAD)


def tok_slice(h):
    return slice(h * TQ, (h + 1) * TQ)


def prep_kernel(x_ref, gain_ref, w_ref, b_ref, cos_ref, sin_ref, h_ref, r_ref, kv_ref):
    rows, d = x_ref.shape
    total = jnp.zeros((rows, HEAD), F32)
    for c in range(0, d, HEAD):
        x = x_ref[:, c:c + HEAD].astype(F32)
        total += x * x
    r = lax.rsqrt(jnp.sum(total, axis=1, keepdims=True) * (1.0 / d) + EPS)
    r_ref[...] = r
    for c in range(0, d, HEAD):
        h_ref[:, c:c + HEAD] = (x_ref[:, c:c + HEAD].astype(F32) * r * gain_ref[:, c:c + HEAD]).astype(BF)
    kv = (mxu(h_ref[...], w_ref[...]) + b_ref[...]).astype(BF)
    k = kv[:, :HEAD].T
    top = k[:ROT].astype(F32)
    turned = (top * cos_ref[...] + swap_pairs(top) * sin_ref[...]).astype(BF)
    kv_ref[:, :HEAD] = jnp.concatenate([turned, k[ROT:]], axis=0).T
    kv_ref[:, HEAD:] = kv[:, HEAD:]


def prep(x, gain, w, bias, cos_t, sin_t, qw):
    tokens, d = x.shape
    tm, kv = 256, 2 * HEAD
    row, tab = rows_of(tm, d), cols_of(ROT, tm)
    return kernel_call(
        prep_kernel, 28, (tokens // tm,),
        [row, once((1, d)), once((d, kv), qw // kv), once((1, kv), qw // kv), tab, tab],
        [row, rows_of(tm, 1), rows_of(tm, kv)],
        [shape((tokens, d), BF), shape((tokens, 1), F32), shape((tokens, kv), BF)],
        (x, gain, w, bias, cos_t, sin_t))


def q_kernel(h_ref, w_ref, b_ref, cos_ref, sin_ref, qt_ref):
    nq = qt_ref.shape[0]
    for n in range(w_ref.shape[1] // COLS):
        c0 = n * COLS
        p = (mxu(h_ref[...], w_ref[:, c0:c0 + COLS]) + b_ref[:, c0:c0 + COLS]).astype(BF)
        for u in range(4):
            hs = slice(u * HEAD, (u + 1) * HEAD)
            for t in range(nq):
                ts = slice(t * TQ, (t + 1) * TQ)
                tile = p[ts, hs].T
                top = tile[:ROT].astype(F32)
                turned = (top * cos_ref[:, ts] + swap_pairs(top) * sin_ref[:, ts]).astype(BF)
                sl = tok_slice(c0 // HEAD + u)
                qt_ref[t, :ROT, sl] = turned
                qt_ref[t, ROT:, sl] = tile[ROT:]


def q_turn_kernel(s_ref, h_ref, w_ref, b_ref, cos_ref, sin_ref, rows_ref, qt_ref, t_ref, half_ref):
    t = rows_ref[...].T
    t_ref[...] = t

    @pl.when(pl.program_id(0) // (pl.num_programs(0) // 2) == s_ref[0] % 2)
    def _():
        half_ref[...] = t

    q_kernel(h_ref, w_ref, b_ref, cos_ref, sin_ref, qt_ref)


def q_project(half, part, parts, whole, h, w, bias, cos_t, sin_t, qw, table=None):
    tokens, d = h.shape
    rows = 512
    nq = rows // TQ
    width = qw // 2
    cols = width // HEAD * TQ
    steps = tokens // rows // parts
    i0 = part * steps
    tab = cols_of(ROT, rows, i0)
    in_specs = [rows_of(rows, d, i0), once((d, width), half), once((1, width), half), tab, tab]
    out_specs = [pl.BlockSpec((nq, HEAD, cols), lambda i, *_: (i + i0, 0, 0))]
    out_shape = [shape((tokens // TQ, HEAD, cols), BF)]
    args = [h, w, bias, cos_t, sin_t]
    body, alias = with_whole(q_kernel, len(args), args, in_specs, whole)
    if table is not None:
        body, nh, all_w = q_turn_kernel, steps // 2, w.shape[1]
        in_specs.append(rows_of(d // steps, all_w))
        out_specs += [cols_of(all_w, d // steps),
                      pl.BlockSpec((all_w, d // steps), lambda i, s: (0, jnp.clip(i - s[0] % 2 * nh, 0, nh - 1)))]
        out_shape += [shape((all_w, d), BF), shape((all_w, d // 2), BF)]
        args = [table, *args, w]

    return kernel_call(body, 42 // parts, (steps,), in_specs, out_specs, out_shape, args, alias=alias, prefetch=int(table is not None))


def for_keys(lo, hi, step):
    def pair(i, _):
        step(pl.multiple_of((lo + 2 * i) * TK, TK), 2 * TK)
        return 0

    lax.fori_loop(0, (hi - lo) // 2, pair, 0)

    @pl.when((hi - lo) % 2 == 1)
    def _():
        step(pl.multiple_of((hi - 1) * TK, TK), TK)


def key_bias(start_ref, q0, k0, n):
    j = k0 + lax.broadcasted_iota(jnp.int32, (n, TQ), 0)
    i = q0 + lax.broadcasted_iota(jnp.int32, (n, TQ), 1)
    return jnp.where((j >= start_ref[0]) & (j <= i), 0.0, NEG).astype(F32)


FLIPS = (0, 2, 1, 3)


def chunk_rows(s_ref, flip, chunk):
    return pl.ds(pl.multiple_of((s_ref[0] ^ flip) * chunk, chunk), chunk)


def of_batch(dims, b0=0):
    return pl.BlockSpec(dims, lambda b, *_: (b + b0, 0, 0))


def start_spec(b0=0):
    return pl.BlockSpec((1, 1, TQ), lambda b, i, *_: (b + b0, 0, i))


def key_range(s_ref, b, t, nq):
    q0 = s_ref[0] * (nq * TQ) + t * TQ
    return q0, s_ref[1 + b * nq + t] // TK, (q0 + TQ - 1) // TK + 1


def fwd_kernel(s_ref, start_ref, qt_ref, kv0_ref, kv1_ref, kv2_ref, kv3_ref, o_ref, ct_ref, lse_ref, k_s, vt_s, t_s, acc_s, m_s, m8_s, l8_s, e_s):
    b, t, nq = pl.program_id(0), pl.program_id(1), pl.num_programs(1)
    heads = qt_ref.shape[2] // TQ

    @pl.when(t == 0)
    def _():
        for ref, flip in zip((kv0_ref, kv1_ref, kv2_ref, kv3_ref), FLIPS):
            rows = chunk_rows(s_ref, flip, ref.shape[1])
            k_s[rows, :] = ref[0, :, :HEAD]
            vt_s[:, rows] = ref[0, :, HEAD:].T

    m8_s[...] = jnp.full_like(m8_s, NEG)
    l8_s[...] = jnp.zeros_like(l8_s)
    acc_s[...] = jnp.zeros_like(acc_s)
    q0, lo, hi = key_range(s_ref, b, t, nq)

    def scores(k0, n):
        rows = pl.ds(k0, n)
        bias = key_bias(start_ref, q0, k0, n)
        k = k_s[rows, :]
        for h in range(heads):
            sl = tok_slice(h)
            s = mxu(k, qt_ref[0, :, sl]) * SCALE2 + bias
            t_s[rows, sl] = s
            m8_s[:, sl] = jnp.maximum(m8_s[:, sl], jnp.max(s.reshape(n // 8, 8, TQ), axis=0))

    for_keys(lo, hi, scores)
    m_s[...] = jnp.max(m8_s[...], axis=0, keepdims=True)

    def accumulate(k0, n):
        rows = pl.ds(k0, n)
        for h in range(heads):
            sl = tok_slice(h)
            e = jnp.exp2(t_s[rows, sl] - m_s[:, sl])
            l8_s[:, sl] += jnp.sum(e.reshape(n // 8, 8, TQ), axis=0)
            e_s[:n, sl] = e.astype(BF)
        acc_s[...] += mxu(vt_s[:, rows], e_s[:n, :])

    for_keys(lo, hi, accumulate)
    l = jnp.sum(l8_s[...], axis=0, keepdims=True)
    lse_ref[0] = m_s[...] + jnp.log2(l)
    l8_s[0:1, :] = 1.0 / l
    for h in range(heads):
        sl = tok_slice(h)
        ct = (acc_s[:, sl] * l8_s[0:1, sl]).astype(BF)
        ct_ref[0, :, sl] = ct
        o_ref[:, head_slice(h)] = ct.T


def attn_fwd(table, start, qt, kvs):
    batch, _, chunk = start.shape
    nq = chunk // TQ
    n, _, cols = qt.shape
    width = cols // TQ * HEAD
    keys = 4 * chunk
    kv, tile = of_batch((1, chunk, 2 * HEAD)), tiles_of((1, HEAD, cols), nq)
    return kernel_call(
        fwd_kernel, 65, (batch, nq),
        [start_spec(), tile, kv, kv, kv, kv],
        [tiles_of((TQ, width), nq), tile, tiles_of((1, 1, cols), nq)],
        [shape((n * TQ, width), BF), shape((n, HEAD, cols), BF), shape((n, 1, cols), F32)], (table, start, qt, *kvs),
        [pltpu.VMEM((keys, HEAD), BF), pltpu.VMEM((HEAD, keys), BF), pltpu.VMEM((keys, cols), F32), pltpu.VMEM((HEAD, cols), F32),
         pltpu.VMEM((1, cols), F32), pltpu.VMEM((8, cols), F32), pltpu.VMEM((8, cols), F32), pltpu.VMEM((2 * TK, cols), BF)],
        prefetch=1)


def bwd_kernel(b0, riding, s_ref, start_ref, qta_ref, qtb_ref, dcta_ref, dctb_ref, cta_ref, ctb_ref, la_ref, lb_ref,
               cos_ref, sin_ref, kv0_ref, kv1_ref, kv2_ref, kv3_ref, *refs):
    nb, nq = pl.num_programs(0), pl.num_programs(1)
    if riding:
        put_sums(pl.program_id(0) * nq + pl.program_id(1), nb * nq, refs[:riding], refs[riding + 6])
    dq_ref, half_ref, *dkv_refs = refs[riding:riding + 6]
    kv_s, kt_s, dct_s, dqt_s, delta_s, ds_s, dsn_s, pn_s, dkvt_s = refs[-9:]
    b, t = pl.program_id(0) + b0, pl.program_id(1)
    heads = dq_ref.shape[1] // HEAD
    chunk = kv0_ref.shape[1]

    @pl.when(t == 0)
    def _():
        for ref, flip in zip((kv0_ref, kv1_ref, kv2_ref, kv3_ref), FLIPS):
            rows = chunk_rows(s_ref, flip, chunk)
            kv_s[rows, :] = ref[0]
            kt_s[:, rows] = ref[0, :, :HEAD].T
        dkvt_s[...] = jnp.zeros_like(dkvt_s)

    def of_head(h, a_ref, b_ref):
        return (a_ref, h) if h < heads // 2 else (b_ref, h - heads // 2)

    for h in range(heads):
        sl = tok_slice(h)
        ref, u = of_head(h, dcta_ref, dctb_ref)
        dct = ref[head_slice(u), :]
        dct_s[:, sl] = dct
        ref, u = of_head(h, cta_ref, ctb_ref)
        delta_s[:, sl] = jnp.sum(dct.astype(F32) * ref[0, :, tok_slice(u)].astype(F32), axis=0, keepdims=True)
    dqt_s[...] = jnp.zeros_like(dqt_s)
    q0, lo, hi = key_range(s_ref, b, t, nq)

    def step(kb, _):
        k0 = pl.multiple_of(kb * TK, TK)
        rows = pl.ds(k0, TK)
        bias = key_bias(start_ref, q0, k0, TK)
        k = kv_s[rows, :HEAD]
        v = kv_s[rows, HEAD:]
        for h in range(heads):
            sl = tok_slice(h)
            qt, u = of_head(h, qta_ref, qtb_ref)
            lse, _ = of_head(h, la_ref, lb_ref)
            us = tok_slice(u)
            p = jnp.exp2(mxu(k, qt[0, :, us]) * SCALE2 + bias - lse[0, :, us])
            ds = (p * (mxu(v, dct_s[:, sl]) - delta_s[:, sl])).astype(BF)
            pn_s[sl, :] = p.astype(BF).T
            dsn_s[sl, :] = ds.T
            ds_s[:, sl] = ds
        dqt_s[...] += mxu(kt_s[:, rows], ds_s[...])
        half = dsn_s.shape[0] // 2
        dkvt_s[:HEAD, rows] += mxu(qta_ref[0], dsn_s[:half, :]) + mxu(qtb_ref[0], dsn_s[half:, :])
        dkvt_s[HEAD:, rows] += mxu(dct_s[...], pn_s[...])
        return 0

    lax.fori_loop(lo, hi, step, 0)
    for h in range(heads):
        sl = tok_slice(h)
        top = dqt_s[:ROT, sl] * SCALE
        turned = top * cos_ref[...] - swap_pairs(top) * sin_ref[...]
        dq = jnp.concatenate([turned, dqt_s[ROT:, sl] * SCALE], axis=0).astype(BF).T
        dq_ref[:, head_slice(h)] = dq
        half_ref[:, head_slice(h)] = dq

    @pl.when(t == nq - 1)
    def _():
        for ref, flip in zip(dkv_refs, FLIPS):
            rows = chunk_rows(s_ref, flip, chunk)
            ref[0, :HEAD, :] = dkvt_s[:HEAD, rows] * SCALE
            ref[0, HEAD:, :] = dkvt_s[HEAD:, rows]


def attn_bwd(half, whole, sums, table, start, qts, dcts, cts, lses, cos_t, sin_t, kvs):
    batch, _, chunk = start.shape
    nq = chunk // TQ
    n, _, cols = qts[0].shape
    width = 2 * dcts[0].shape[0]
    keys = 4 * chunk
    nb = batch // 2
    b0 = half * nb
    kv, tile, line = of_batch((1, chunk, 2 * HEAD), b0), tiles_of((1, HEAD, cols), nq, b0), tiles_of((1, 1, cols), nq, b0)
    dct, tab = tile_cols(width // 2, nq, b0), tile_cols(ROT, nq, b0)
    one, one_spec = shape((nb, 2 * HEAD, chunk), F32), of_batch((1, 2 * HEAD, chunk))
    in_specs = [start_spec(b0), tile, tile, dct, dct, tile, tile, line, line, tab, tab] + [kv] * 4
    args = [table, start, *qts, *dcts, *cts, *lses, cos_t, sin_t, *kvs]
    out_specs = [tiles_of((TQ, width), nq, b0), tiles_of((TQ, width), nq)] + [one_spec] * 4
    out_shape = [shape((n * TQ, width), BF), shape((n * TQ // 2, width), BF)] + [one] * 4
    if sums:
        specs, block, put = ride(nb * nq, lambda b, i, s: b * nq + i, lambda core: core, sums)
        in_specs += specs
        args += sums
        out_specs.append(pl.BlockSpec(block, lambda *g: (put(*g), 0)))
        out_shape.append(shape((4 * sums[0].shape[0], block[1]), F32))
    body, alias = with_whole(functools.partial(bwd_kernel, b0, len(sums)), len(args), args, in_specs, whole)
    return kernel_call(
        body, 80, (nb, nq), in_specs, out_specs, out_shape, args,
        [pltpu.VMEM((keys, 2 * HEAD), BF), pltpu.VMEM((HEAD, keys), BF), pltpu.VMEM((HEAD, 2 * cols), BF),
         pltpu.VMEM((HEAD, 2 * cols), F32), pltpu.VMEM((1, 2 * cols), F32), pltpu.VMEM((TK, 2 * cols), BF),
         pltpu.VMEM((2 * cols, TK), BF), pltpu.VMEM((2 * cols, TK), BF), pltpu.VMEM((2 * HEAD, keys), F32)],
        prefetch=1, alias=alias)


def first_tile(total, a_s, b_s, w_ref, piece_refs, places, w_s, p_s, sems):
    n = w_s.shape[0] // 256
    part = piece_refs[0].shape[1]

    def copies(k):
        rows = pl.ds(pl.multiple_of(k * 256, 256), 256)
        moves = [(w_ref.at[rows, :], w_s.at[rows, :])]
        moves += [(ref.at[rows, :], p_s.at[rows, pl.ds(pl.multiple_of(c * part, part), part)]) for ref, c in zip(piece_refs, places)]
        return [pltpu.make_async_copy(src, dst, sems.at[u, k]) for u, (src, dst) in enumerate(moves)]

    ahead = 3
    for k in range(ahead):
        for copy in copies(k):
            copy.start()
    total[...] = jnp.zeros_like(total)

    def add(k, _):
        for copy in copies(k):
            copy.wait()

        @pl.when(k + ahead < n)
        def _():
            for copy in copies(k + ahead):
                copy.start()

        rows = pl.ds(pl.multiple_of(k * 256, 256), 256)
        for c in range(0, total.shape[1], COLS):
            cs = slice(c, c + COLS)
            total[:, cs] += mxu(a_s[:, rows], w_s[rows, cs]) + mxu(b_s[:, rows], p_s[rows, cs])
        return 0

    lax.fori_loop(0, n, add, 0)


def out_kernel(s_ref, x_ref, ca_ref, cb_ref, pa_ref, pb_ref, w_ref, p0_ref, p1_ref, p2_ref, p3_ref, *refs):
    put_ref, o_ref, w_s, p_s, c_s, d_s, total_s, sems = refs[-8:]
    put_sums(pl.program_id(0), pl.num_programs(0), refs[:-8], put_ref)
    k = ca_ref.shape[1]
    first = pl.program_id(0) == 0
    c_s[:, :k], c_s[:, k:] = ca_ref[...], cb_ref[...]
    d_s[:, :k], d_s[:, k:] = pa_ref[...], pb_ref[...]

    def finish(cs, acc):
        o_ref[:, cs] = (x_ref[:, cs].astype(F32) + acc).astype(BF)

    tiles = [slice(c, c + COLS) for c in range(0, o_ref.shape[1], COLS)]

    @pl.when(first)
    def _():
        first_tile(total_s, c_s, d_s, w_ref, (p0_ref, p1_ref, p2_ref, p3_ref), [s_ref[0] ^ flip for flip in (0, 2, 1, 3)], w_s, p_s, sems)
        for cs in tiles:
            finish(cs, total_s[:, cs])

    @pl.when(jnp.logical_not(first))
    def _():
        for cs in tiles:
            finish(cs, mxu(c_s[...], w_s[:, cs]) + mxu(d_s[...], p_s[:, cs]))


def out_project(table, x, ctx, peer, w, pieces, sums, whole):
    tokens, d = x.shape
    k = w.shape[0]
    tm = 256
    n = tokens // tm
    row, crow = rows_of(tm, d), rows_of(tm, k // 2)
    specs, block, put = ride(n, lambda i, s: i, lambda core: 2 + core, sums)
    in_specs = [row, crow, crow, crow, crow] + [ANYWHERE] * 5 + specs
    args = [table, x, *ctx, *peer, w, *pieces, *sums]
    body, alias = with_whole(out_kernel, len(args), args, in_specs, [whole])
    return kernel_call(
        body, 150, (n,), in_specs, [pl.BlockSpec(block, lambda *g: (put(*g), 0)), row],
        [shape(whole.shape, F32), shape((tokens, d), BF)], args,
        [pltpu.VMEM((k, d), BF), pltpu.VMEM((k, d), BF), pltpu.VMEM((tm, k), BF), pltpu.VMEM((tm, k), BF), pltpu.VMEM((tm, d), F32),
         pltpu.SemaphoreType.DMA((5, k // 256))], prefetch=1, alias=alias)


def finish_kernel(a_ref, b_ref, c_ref, cos_ref, sin_ref, o_ref):
    dkv = a_ref[0] + b_ref[0] + c_ref[0]
    top = dkv[:ROT]
    turned = top * cos_ref[...] - swap_pairs(top) * sin_ref[...]
    o_ref[...] = jnp.concatenate([turned, dkv[ROT:]], axis=0).astype(BF).T


def finish_dkv(half, own, core, away, cos_t, sin_t):
    nb, width, chunk = own.shape
    one, tab = of_batch((1, width, chunk)), cols_of(ROT, chunk, half * nb)
    return kernel_call(
        finish_kernel, 4, (nb,), [one, one, one, tab, tab], rows_of(chunk, width),
        shape((nb * chunk, width), BF), (own, core, away, cos_t, sin_t))


def dh_kernel(s_ref, x_ref, g_ref, r_ref, gain_ref, qa_ref, ka_ref, qb_ref, kb_ref, w_ref, p0_ref, p1_ref,
              gx_ref, gg_ref, gb_ref, dh_s, gg8_s, gb8_s, w_s, p_s, a_s, b_s, sems):
    i = pl.program_id(0)
    qw = qa_ref.shape[1]
    tm, d = x_ref.shape
    a_s[:, :qw], a_s[:, qw:] = qa_ref[...], ka_ref[...]
    b_s[:, :qw], b_s[:, qw:] = qb_ref[...], kb_ref[...]

    @pl.when(i == 0)
    def _():
        gg8_s[...] = jnp.zeros_like(gg8_s)
        gb8_s[...] = jnp.zeros_like(gb8_s)
        core = s_ref[0] % 2
        first_tile(dh_s, a_s, b_s, w_ref, (p0_ref, p1_ref), (core, 1 - core), w_s, p_s, sems)

    @pl.when(i > 0)
    def _():
        for c in range(0, d, COLS):
            cs = slice(c, c + COLS)
            dh_s[:, cs] = mxu(a_s[...], w_s[:, cs]) + mxu(b_s[...], p_s[:, cs])

    def norm(k, _):
        n = 128
        rs = pl.ds(pl.multiple_of(k * n, n), n)
        r = jnp.broadcast_to(r_ref[rs, :], (n, HEAD))
        total = jnp.zeros((n, HEAD), F32)
        for c in range(0, d, HEAD):
            cs = slice(c, c + HEAD)
            prod = dh_s[rs, cs] * (x_ref[rs, cs].astype(F32) * r)
            gg8_s[:, cs] += jnp.sum(prod.reshape(n // 8, 8, HEAD), axis=0)
            total += prod * gain_ref[:, cs]
        mean = jnp.sum(total, axis=1, keepdims=True) * (1.0 / d)
        r_mean = jnp.broadcast_to(r_ref[rs, :] * mean, (n, HEAD))
        for c in range(0, d, HEAD):
            cs = slice(c, c + HEAD)
            part_x = dh_s[rs, cs] * gain_ref[:, cs] - x_ref[rs, cs].astype(F32) * r_mean
            gx_ref[rs, cs] = (g_ref[rs, cs].astype(F32) + r * part_x).astype(BF)
        for c in range(0, a_s.shape[1], HEAD):
            cs = slice(c, c + HEAD)
            gb8_s[:, cs] += jnp.sum(a_s[rs, cs].astype(F32).reshape(n // 8, 8, HEAD), axis=0)
        return 0

    lax.fori_loop(0, tm // 128, norm, 0, unroll=True)

    @pl.when(i == pl.num_programs(0) - 1)
    def _():
        gg_ref[...] = jnp.sum(gg8_s[...], axis=0, keepdims=True)
        gb_ref[...] = jnp.sum(gb8_s[...], axis=0, keepdims=True)


def dh_norm(half, whole, table, x, g, r, gain, qa, ka, qb, kb, wt, pieces):
    tokens, d = x.shape
    tm = 256
    nt = tokens // tm // 2
    i0 = half * nt
    qw, kw = qa.shape[1], ka.shape[1]
    row = rows_of(tm, d, i0)
    in_specs = [row, row, rows_of(tm, 1, i0), once((1, d)), rows_of(tm, qw, i0), rows_of(tm, kw), rows_of(tm, qw), rows_of(tm, kw)] + [ANYWHERE] * 3
    args = [table, x, g, r, gain, qa, ka, qb, kb, wt, *pieces]
    body, alias = with_whole(dh_kernel, len(args), args, in_specs, whole)
    all_w = qw + kw
    return kernel_call(
        body, 100, (nt,), in_specs, [row, once((1, d)), once((1, all_w))],
        [shape((tokens, d), BF), shape((1, d), F32), shape((1, all_w), F32)], args,
        [pltpu.VMEM((tm, d), F32), pltpu.VMEM((8, d), F32), pltpu.VMEM((8, all_w), F32), pltpu.VMEM((all_w, d), BF), pltpu.VMEM((all_w, d), BF),
         pltpu.VMEM((tm, all_w), BF), pltpu.VMEM((tm, all_w), BF), pltpu.SemaphoreType.DMA((3, all_w // 256))],
        prefetch=1, alias=alias)


def place_kernel(s_ref, a_ref, b_ref, c_ref, d_ref, o_ref):
    put_sums(pl.program_id(0), pl.num_programs(0), (a_ref, b_ref, c_ref, d_ref), o_ref)


def place(table, sums, quarter, column, whole, dims):
    steps = max(4, sums[0].shape[1] // 256)
    in_specs, block, put = ride(steps, lambda i, s: i, quarter, sums)
    args = [table, *sums]
    body, alias = with_whole(place_kernel, len(args), args, in_specs, whole)
    return kernel_call(
        body, 20, (steps,), in_specs, pl.BlockSpec(block, lambda *g: (put(*g), column)), shape(dims, F32), args, prefetch=1, alias=alias)


def solution(mesh):
    over_tp = [(i, 1 - i) for i in range(2)]
    over_x = [(i, i ^ 2) for i in range(4)]
    over_core = [(i, i ^ 1) for i in range(4)]

    def send_tp(v):
        return lax.ppermute(v, 'tp', over_tp)

    def send_x(v, pairs=over_x):
        return lax.ppermute(v, 'cp', pairs)

    def send_core(v):
        return lax.ppermute(v, 'cp', over_core)

    def body(x_blk, grad_blk, norm_gain, w_qkv, b_qkv, w_out, doc_blk, pos_blk):
        batch, chunk, d = x_blk.shape
        tokens = batch * chunk
        qw = w_out.shape[0]
        cp = lax.axis_index('cp')
        core = cp % 2
        x = x_blk.reshape(tokens, d)
        g = grad_blk.reshape(tokens, d)
        gain = norm_gain[None].astype(F32)
        bias = b_qkv[None].astype(F32)

        start = cp * chunk + jnp.arange(chunk, dtype=jnp.int32)[None] - pos_blk
        table = jnp.concatenate([cp[None].astype(jnp.int32), start[:, ::TQ].reshape(-1)])
        start = start[:, None, :]
        me = table[:1]

        inv_freq = 1.0 / ROPE_BASE ** (jnp.arange(0, ROT, 2, dtype=F32) / ROT)
        angles = pos_blk.reshape(1, tokens).astype(F32) * jnp.repeat(inv_freq, 2)[:, None]
        sign = jnp.where(jnp.arange(ROT) % 2 == 0, -1.0, 1.0)[:, None]
        cos_t = jnp.cos(angles)
        sin_t = jnp.sin(angles) * sign

        wo0 = send_tp(lax.dynamic_slice_in_dim(w_out, cp * (d // 4), d // 4, 1))
        h, inv_rms, kv = prep(x, gain, w_qkv, bias, cos_t, sin_t, qw)
        kv_own = kv.reshape(batch, chunk, 2 * HEAD)
        kv_x = send_x(kv_own, over_x[:2])
        kvs = (kv_own, kv_x, send_core(kv_own), send_core(kv_x))
        q_args = (h, w_qkv, bias, cos_t, sin_t, qw)
        qta, wq_t, wq_half = q_project(0, 0, 1, None, *q_args, table=me)
        wq0 = send_tp(wq_half)
        wo1 = send_x(wo0)
        wo_pieces = (wo0, wo1, send_core(wo0), send_core(wo1))
        wq_pieces = (wq0, send_core(wq0))

        ctx_a, ct_a, lse_a = attn_fwd(table, start, qta, kvs)
        qtb, = q_project(1, 1, 2, q_project(1, 0, 2, None, *q_args), *q_args)
        ctx_b, ct_b, lse_b = attn_fwd(table, start, qtb, kvs)
        peer_ctx = (send_tp(ctx_a), send_tp(ctx_b))

        def part(lhs, rhs, first, k):
            cols = lax.dynamic_slice_in_dim(lhs, first * k, k, 1)
            return lax.dot_general(cols, rhs, (((0,), (0,)), ((), ())), preferred_element_type=F32)

        def across(v):
            other = send_x(v)
            return [v, other, send_core(v), send_core(other)]

        go = []
        for ctx in (ctx_a, ctx_b):
            k = ctx.shape[1] // 2
            got = send_core(part(ctx, g, 1 - core, k))
            mine = part(ctx, g, core, k) + got
            go.append(across(mine))

        def grad_ctx(w):
            return lax.dot_general(w, g, (((1,), (1,)), ((), ())), preferred_element_type=F32).astype(BF)

        dctx_t = (grad_ctx(w_out[:qw // 2]), grad_ctx(w_out[qw // 2:]))

        attn_args = (table, start, (qta, qtb), dctx_t, (ct_a, ct_b), (lse_a, lse_b), cos_t, sin_t, kvs)

        def own_dkv(half, own, away, core, both):
            away = away + send_core(both)
            core = send_core(core)
            return finish_dkv(half, own, core, send_x(away, over_x[2:]), cos_t, sin_t)

        dq, dq_a, *dkv_parts, gw_out = attn_bwd(0, None, go[0], *attn_args)
        dqp_a = send_tp(dq_a)
        dkv_a = own_dkv(0, *dkv_parts)
        dq, dq_b, *dkv_parts = attn_bwd(1, [dq], [], *attn_args)
        dqp_b = send_tp(dq_b)
        dkv_b = own_dkv(1, *dkv_parts)
        dkvp_a = send_tp(dkv_a)
        dkvp_b = send_tp(dkv_b)
        dkv = jnp.concatenate([dkv_a, dkv_b], axis=0)

        k = d // 4
        got = [send_core(part(h, dq, 2 * (1 - core) + i, k)) for i in range(2)]
        mine = [part(h, dq, 2 * core + i, k) + got[i] for i in range(2)]
        gq = [across(mine[i]) for i in range(2)]
        got = send_core(part(h, dkv, 1 - core, 2 * k))
        gkv = across(part(h, dkv, core, 2 * k) + got)
        dims = (d, w_qkv.shape[1])
        gw_qkv = place(me, gq[0], lambda core: 2 * core, 0, None, dims)
        gw_qkv = place(me, gq[1], lambda core: 2 * core + 1, 0, [gw_qkv], dims)
        gw_qkv = place(me, gkv, lambda core: core, qw // gkv[0].shape[1], [gw_qkv], dims)

        gw_out, out = out_project(me, x, (ctx_a, ctx_b), peer_ctx, w_out, wo_pieces, go[1], gw_out)

        dh_args = (me, x, g, inv_rms, gain, dq)
        grad_x, gain_a, bias_a = dh_norm(0, None, *dh_args, dkv_a, dqp_a, dkvp_a, wq_t, wq_pieces)
        grad_x, gain_b, bias_b = dh_norm(1, [grad_x], *dh_args, dkv_b, dqp_b, dkvp_b, wq_t, wq_pieces)
        nb = bias_a.shape[1]
        small = jnp.concatenate([bias_a + bias_b, gain_a + gain_b], axis=1).reshape(-1, HEAD)
        small = small + send_core(small)
        small = (small + send_x(small)).reshape(-1)
        return out.reshape(x_blk.shape), grad_x.reshape(x_blk.shape), small[nb:], gw_qkv, small[:nb], gw_out

    seq, rep, cols = P(None, 'cp', None), P(), P(None, 'tp')
    specs_in = (seq, seq, rep, cols, P('tp'), P('tp', None), P(None, 'cp'), P(None, 'cp'))
    specs_out = (seq, seq, rep, cols, P('tp'), P('tp', None))
    return jax.shard_map(body, mesh=mesh, in_specs=specs_in, out_specs=specs_out, check_vma=False)
```
